32 devices in a mesh: gx: 4 (over y, core), gy: 2 (over x), gz: 4 (over z).
Axes of the slice: x: 2, y: 2, z: 4, core: 2. Of those that a mesh axis runs over, the one named last changes fastest.
Arguments:
- positions: float32 [4, 2, 8, 3, 128], P('gx', 'gy', 'gz'), may hold values from 0 to 256, as said below
- gaussian: float32 [4, 2, 8, 3, 128], P('gx', 'gy', 'gz'), may hold values from -120 to 120
- counts: int32 [4, 2, 8], P('gx', 'gy', 'gz'), may hold values from 32 to 128, as said below
Outputs:
- brownian: float32 [4, 2, 8, 3, 128], P('gx', 'gy', 'gz')
The draws below stay inside these ranges and needn't reach their ends.
Inputs may be any that keep to these rules, and one draw needn't show every extreme that they name: `positions`: slot k of a cell lies within a quarter of 4 of its own lattice point in each component; the lattice points of all slots of all cells have spacing 4 and the cell of index (a, b, e) spans 4 points along the first two dimensions and 8 along the third from index 0 upward. Each cell's live particles are its first counts slots; every cell of the wall layer (third cell index 0) is full.
All inputs are finite; a program needn't handle non-finite values.
Results may differ from the reference program's by a relative error of at most 0.0003.
Values sent between devices are 32-bit elements; how exact they have to be, the bound alone decides.
A program may use at most 64 MiB of HBM per device.

```python
import jax
import jax.numpy as jnp
from jax import lax

P_SIZE = 128
NCX = 4
NCY = 2
NCZ = 8


spacing = 4.0


def cell_index():
    grids = jnp.meshgrid(jnp.arange(NCX), jnp.arange(NCY), jnp.arange(NCZ), indexing='ij')
    return [grid.astype(jnp.float32) for grid in grids]


def draw_positions(key, part):
    slot_index = jnp.arange(P_SIZE)
    lattice_site = jnp.stack([slot_index % 4, slot_index // 4 % 4, slot_index // 16]).astype(jnp.float32)
    grids = cell_index()
    cell_extent = jnp.array([4.0, 4.0, float(P_SIZE // 16)], dtype=jnp.float32)
    cell_corner = jnp.stack(grids, axis=-1) * cell_extent
    lattice = (cell_corner[..., None] + lattice_site + 0.5) * spacing
    full_shape = (NCX, NCY, NCZ, 3, P_SIZE)
    jitter = jnp.clip(0.1 * jax.random.normal(key, full_shape), -0.25, 0.25)
    return lattice + jitter * spacing


def draw_gaussian(key, part):
    grids = cell_index()
    factor = (1.0 + 2.0 * grids[0] / max(NCX - 1, 1)) * (1.0 + 2.0 * grids[1] / max(NCY - 1, 1)) * (1.0 + 2.0 * grids[2] / max(NCZ - 1, 1))
    spread = jnp.sqrt(factor)[:, :, :, None, None]
    full_shape = (NCX, NCY, NCZ, 3, P_SIZE)
    first_key = jax.random.fold_in(jax.random.fold_in(key, 17), 0)
    return jnp.clip(jax.random.normal(first_key, full_shape), -6.0, 6.0) * spread


def draw_counts(key, part):
    layer = jnp.broadcast_to(jnp.arange(NCZ, dtype=jnp.int32)[None, None, :], (NCX, NCY, NCZ))
    reach = 3 * P_SIZE // 4 * layer // max(NCZ - 1, 1)
    removed = jax.random.randint(jax.random.fold_in(key, 29), (NCX, NCY, NCZ), 0, reach + 1)
    return (P_SIZE - removed).astype(jnp.int32)


def setup_inputs(seed: int = 0) -> dict:
    seeds = jax.random.split(jax.random.key(seed), 4)
    return {
        "positions": draw_positions(jax.random.fold_in(seeds[3], 71), 0),
        "gaussian": draw_gaussian(jax.random.fold_in(seeds[3], 71), 0),
        "counts": draw_counts(jax.random.fold_in(seeds[3], 71), 0),
    }


wall_gap = 1.0
cell_offsets = ((0, 0, 0), (1, 0, 0), (-1, 0, 0), (0, 1, 0), (0, -1, 0), (0, 0, 1), (0, 0, -1))

def pair_terms(target, source, values, self_pair):
    offset_vec = target[:, :, :, None] - source[:, :, None, :]
    distance_sq = lax.optimization_barrier(jnp.sum(offset_vec * offset_vec, axis=1))
    width = target.shape[-1]
    diagonal = jnp.eye(width, dtype=bool)[None]
    if self_pair:
        distance_sq = jnp.where(diagonal, 1.0, distance_sq)
    inverse = lax.rsqrt(distance_sq)
    inv_cube = inverse * inverse * inverse
    isotropic = 0.75 * inverse + 0.5 * inv_cube
    dyadic = (0.75 * inverse - 1.5 * inv_cube) * inverse * inverse
    if self_pair:
        isotropic = jnp.where(diagonal, 0.0, isotropic)
        dyadic = jnp.where(diagonal, 0.0, dyadic)
    projected = lax.optimization_barrier(jnp.sum(offset_vec * values[:, :, None, :], axis=1))
    direct = jnp.einsum('bij,bcj->bci', isotropic, values, precision=lax.Precision.HIGHEST)
    along_pair = lax.optimization_barrier(jnp.sum(offset_vec * (dyadic * projected)[:, None], axis=3))
    return direct + along_pair

def wall_self(target, values):
    inv_height = 1.0 / (target[:, 2] + wall_gap)
    squared = inv_height * inv_height
    cubed = squared * inv_height
    fourth = squared * squared
    fifth = fourth * inv_height
    eleventh = fifth * fifth * inv_height
    twelfth = eleventh * inv_height
    parallel = 1.0 - 0.5625 * inv_height + 0.125 * cubed - 0.17578125 * fourth - 0.0625 * fifth
    perpend = 1.0 - 1.125 * inv_height + 0.5 * cubed - 0.57 * fourth + 0.2 * fifth + 0.035 * eleventh - 0.04 * twelfth
    mobility = jnp.stack([parallel, parallel, perpend], axis=1)
    return mobility * values

def cell_block(operands):
    target, sources, vectors, occupied = operands
    summed = wall_self(target, vectors[0])
    for neighbour in range(7):
        summed = summed + pair_terms(target, sources[neighbour], vectors[neighbour], neighbour == 0)
    return summed * occupied[:, None, :]

def stacked(padded, size_x, size_y, size_z):
    pieces = []
    for shift_x, shift_y, shift_z in cell_offsets:
        piece = padded[1 + shift_x:1 + shift_x + size_x, 1 + shift_y:1 + shift_y + size_y, 1 + shift_z:1 + shift_z + size_z]
        pieces.append(piece.reshape((size_x * size_y, size_z) + piece.shape[3:]))
    return jnp.stack(pieces, axis=1)

def apply_mobility(padded_pos, padded_vec, occupied):
    size_x, size_y, size_z = (occupied.shape[0], occupied.shape[1], occupied.shape[2])
    width = occupied.shape[3]
    target = padded_pos[1:-1, 1:-1, 1:-1].reshape((size_x * size_y, size_z, 3, width))
    sources = stacked(padded_pos, size_x, size_y, size_z)
    vectors = stacked(padded_vec, size_x, size_y, size_z)
    live = occupied.reshape((size_x * size_y, size_z, width))
    result = lax.map(cell_block, (target, sources, vectors, live))
    return result.reshape((size_x, size_y, size_z, 3, width))

def padding(field):
    return jnp.pad(field, ((1, 1), (1, 1), (1, 1), (0, 0), (0, 0)))

def reference(positions, gaussian, counts):
    slot_index = jnp.arange(P_SIZE, dtype=jnp.int32)
    occupied = (slot_index[None, None, None, :] < counts[:, :, :, None]).astype(jnp.float32)
    masked = gaussian * occupied[:, :, :, None, :]
    padded_pos = padding(positions)

    def mobility(vector):
        return apply_mobility(padded_pos, padding(vector), occupied)
    scale = jnp.sqrt(jnp.sum(masked * masked))
    basis_one = masked / scale
    mapped = mobility(basis_one)
    alpha_one = jnp.sum(basis_one * mapped)
    residual = mapped - alpha_one * basis_one
    beta_sq = jnp.sum(residual * residual)
    beta_one = jnp.sqrt(beta_sq)
    basis_two = residual / beta_one
    alpha_two = jnp.sum(basis_two * mobility(basis_two))
    root_det = jnp.sqrt(alpha_one * alpha_two - beta_sq)
    trace_root = jnp.sqrt(alpha_one + alpha_two + 2.0 * root_det)
    return scale * ((alpha_one + root_det) / trace_root * basis_one + beta_one / trace_root * basis_two)
```

```python
import functools
import itertools

import jax
import jax.numpy as jnp
from jax import lax
from jax.experimental import pallas as pl
from jax.experimental.pallas import tpu as pltpu
from jax.sharding import PartitionSpec as P

wall_gap = 1.0
lanes = 8
direct_limit = 64
far_away = -4096.0
names = ("gx", "gy", "gz")


def groups_of(sizes):
    total = sizes[0] * sizes[1] * sizes[2]
    return [(0, 1, 2)] if total <= direct_limit else [(0,), (1,), (2,)]


def stage_offsets(sizes, axes):
    ranges = [range(sizes[k]) if k in axes else range(1) for k in range(3)]
    return [offset for offset in itertools.product(*ranges) if any(offset)]


def shifted(here, sizes, offset):
    return tuple(
        lax.rem(here[k] + offset[k], sizes[k]) if offset[k] else here[k] for k in range(3)
    )


def wall_mobility(height):
    inv_height = 1.0 / (height + wall_gap)
    squared = inv_height * inv_height
    cubed = squared * inv_height
    fourth = squared * squared
    fifth = fourth * inv_height
    eleventh = fifth * fifth * inv_height
    twelfth = eleventh * inv_height
    parallel = 1.0 - 0.5625 * inv_height + 0.125 * cubed - 0.17578125 * fourth - 0.0625 * fifth
    perpend = (
        1.0
        - 1.125 * inv_height
        + 0.5 * cubed
        - 0.57 * fourth
        + 0.2 * fifth
        + 0.035 * eleventh
        - 0.04 * twelfth
    )
    return parallel, parallel, perpend


def kernel(
    sizes, local, width, counts_ref, pos_ref, gauss_ref, out_ref,
    packed, mapped, halo_x, halo_y, halo_z, next_x, next_y, next_z,
    column, image_column, acc, iso, dyad, sums,
    send_one, recv_one, send_two, recv_two, send_sum, recv_sum,
):
    here = tuple(lax.axis_index(name) for name in names)
    cells = list(itertools.product(*(range(size) for size in local)))
    halos, nexts = (halo_x, halo_y, halo_z), (next_x, next_y, next_z)
    stages = groups_of(sizes)
    offsets = [stage_offsets(sizes, axes) for axes in stages]
    faces = [(axis, side) for axis in range(3) if sizes[axis] > 1 for side in range(2)]
    groups = width // lanes

    def exists(axis, side):
        return here[axis] < sizes[axis] - 1 if side else here[axis] > 0

    def slab(axis, side):
        index = [slice(None)] * 3
        index[axis] = pl.ds(local[axis] - 1 if side else 0, 1)
        return tuple(index)

    def beside(axis, side):
        return {names[axis]: here[axis] + (1 if side else -1)}

    zero_tile = jnp.zeros((lanes, width), jnp.float32)
    tile_row = lax.broadcasted_iota(jnp.int32, (lanes, width), 0)
    outside = jnp.where(tile_row < 3, far_away, 0.0)
    for axis in range(3):
        face_cells = [c for c in cells if c[axis] == 0]
        for side in range(2):
            def clear(axis=axis, side=side, face_cells=face_cells):
                for cell in face_cells:
                    halos[axis][(side,) + cell] = outside
                    if side:
                        nexts[axis][cell] = zero_tile
            pl.when(jnp.logical_not(exists(axis, side)))(clear)

    barrier = pltpu.get_barrier_semaphore()
    peers = [offset for stage in offsets for offset in stage]
    for offset in peers:
        pl.semaphore_signal(
            barrier, inc=1, device_id=shifted(here, sizes, offset),
            device_id_type=pl.DeviceIdType.MESH,
        )

    lane = lax.broadcasted_iota(jnp.int32, (1, width), 1)
    occupied, walls = {}, {}
    for cell in cells:
        occupied[cell] = (lane < counts_ref[cell]).astype(jnp.float32)
        position = pos_ref[cell]
        packed[cell + (pl.ds(0, 3),)] = position
        packed[cell + (pl.ds(3, 3),)] = gauss_ref[cell] * occupied[cell]
        packed[cell + (pl.ds(6, 2),)] = jnp.zeros((2, width), jnp.float32)
        walls[cell] = wall_mobility(position[2:3])

    def row(ref, index, which):
        return ref[index + (pl.ds(which, 1),)]

    def spread(ref, cell, values):
        for which in range(3):
            full = jnp.broadcast_to(values[which], (width, width))
            ref[cell + (which,)] = full.T

    for cell in cells:
        spread(column, cell, [row(packed, cell, which) for which in range(3)])

    def source_of(cell, axis, side):
        there = list(cell)
        there[axis] += 1 if side else -1
        if 0 <= there[axis] < local[axis]:
            return packed, tuple(there), False
        there[axis] = 0
        return halos[axis], (side,) + tuple(there), True

    inner, outer, saved = {}, {}, []
    for cell in cells:
        inner[cell] = [(packed, cell, None)]
        outer[cell] = []
        saved.append((cell, None))
        for axis in range(3):
            for side in range(2):
                ref, index, remote = source_of(cell, axis, side)
                if remote and sizes[axis] == 1:
                    continue
                (outer if remote else inner)[cell].append((ref, index, (axis, side)))
                if side:
                    saved.append((cell, axis))
    slot_of = {key: slot for slot, key in enumerate(saved)}

    def diagonal(group):
        rows = group * lanes + lax.broadcasted_iota(jnp.int32, (lanes, width), 0)
        return rows == lax.broadcasted_iota(jnp.int32, (lanes, width), 1)

    def first_product(table, start):
        def body(group, carry):
            rows = pl.ds(pl.multiple_of(group * lanes, lanes), lanes)
            for cell in cells:
                target = [column[cell + (which, rows)] for which in range(3)]
                total = None if start else [acc[cell + (which, rows)] for which in range(3)]
                for ref, index, direction in table[cell]:
                    delta = [target[which] - row(ref, index, which) for which in range(3)]
                    value = [row(ref, index, 3 + which) for which in range(3)]
                    square = delta[0] * delta[0] + delta[1] * delta[1] + delta[2] * delta[2]
                    inverse = lax.rsqrt(square)
                    if direction is None:
                        inverse = jnp.where(diagonal(group), 0.0, inverse)
                    inv_sq = inverse * inverse
                    isotropic = inverse * (0.75 + 0.5 * inv_sq)
                    dyadic = (inverse * inv_sq) * (0.75 - 1.5 * inv_sq)
                    if direction is None or direction[1]:
                        slot = slot_of[(cell, None if direction is None else direction[0])]
                        iso[slot, rows] = isotropic
                        dyad[slot, rows] = dyadic
                    scaled = dyadic * (
                        delta[0] * value[0] + delta[1] * value[1] + delta[2] * value[2]
                    )
                    part = [isotropic * value[which] + delta[which] * scaled for which in range(3)]
                    total = part if total is None else [a + b for a, b in zip(total, part)]
                for which in range(3):
                    acc[cell + (which, rows)] = total[which]
            return carry

        lax.fori_loop(0, groups, body, 0)

    first_product(inner, True)

    pl.semaphore_wait(barrier, len(peers))

    def halo_copy(axis, side, receiver):
        held = side if receiver else 1 - side
        face = 2 * axis + held
        return pltpu.make_async_remote_copy(
            src_ref=packed.at[slab(axis, side)],
            dst_ref=halos[axis].at[held],
            send_sem=send_one.at[2 * axis + side],
            recv_sem=recv_one.at[face],
            device_id=beside(axis, side),
            device_id_type=pl.DeviceIdType.MESH,
        )

    def next_copy(axis, side):
        return pltpu.make_async_remote_copy(
            src_ref=mapped.at[slab(axis, 0)],
            dst_ref=nexts[axis],
            send_sem=send_two.at[axis],
            recv_sem=recv_two.at[axis],
            device_id=beside(axis, side),
            device_id_type=pl.DeviceIdType.MESH,
        )

    for axis, side in faces:
        pl.when(exists(axis, side))(lambda a=axis, s=side: halo_copy(a, s, False).start())
    for axis, side in faces:
        pl.when(exists(axis, side))(lambda a=axis, s=side: halo_copy(a, s, True).wait_recv())

    first_product(outer, False)

    images = {}
    for cell in cells:
        images[cell] = []
        for which in range(3):
            summed = jnp.sum(acc[cell + (which,)].T, axis=0, keepdims=True)
            value = row(packed, cell, 3 + which)
            image = (walls[cell][which] * value + summed) * occupied[cell]
            images[cell].append(image)
            mapped[cell + (pl.ds(which, 1),)] = image
        mapped[cell + (pl.ds(3, lanes - 3),)] = jnp.zeros((lanes - 3, width), jnp.float32)

    for axis in range(3):
        if sizes[axis] > 1:
            pl.when(exists(axis, 0))(lambda a=axis: next_copy(a, 0).start())

    for cell in cells:
        spread(image_column, cell, images[cell])

    def other_of(cell, axis):
        there = list(cell)
        if axis is None:
            return packed, cell, mapped, cell
        there[axis] += 1
        if there[axis] < local[axis]:
            return packed, tuple(there), mapped, tuple(there)
        there[axis] = 0
        return halos[axis], (1,) + tuple(there), nexts[axis], tuple(there)

    blocks = [
        key for key in saved
        if key[1] is None or key[0][key[1]] + 1 < local[key[1]] or sizes[key[1]] > 1
    ]

    def second_body(group, carry):
        rows = pl.ds(pl.multiple_of(group * lanes, lanes), lanes)
        result = []
        for (cell, axis), total in zip(blocks, carry):
            place, index, _, _ = other_of(cell, axis)
            slot = slot_of[(cell, axis)]
            delta = [
                column[cell + (which, rows)] - row(place, index, which) for which in range(3)
            ]
            value = [image_column[cell + (which, rows)] for which in range(3)]
            isotropic = iso[slot, rows]
            scaled = dyad[slot, rows] * (
                delta[0] * value[0] + delta[1] * value[1] + delta[2] * value[2]
            )
            result.append(tuple(
                total[which] + isotropic * value[which] + delta[which] * scaled
                for which in range(3)
            ))
        return tuple(result)

    zero = (jnp.zeros((lanes, width), jnp.float32),) * 3
    pushed = lax.fori_loop(0, groups, second_body, (zero,) * len(blocks))

    noise_sq = cross_one = image_sq = wall_sq = jnp.zeros((1, width), jnp.float32)
    for cell in cells:
        for which in range(3):
            value, image = row(packed, cell, 3 + which), images[cell][which]
            noise_sq += value * value
            cross_one += value * image
            image_sq += image * image
            wall_sq += walls[cell][which] * image * image

    own_pairs = jnp.zeros((lanes, width), jnp.float32)
    remote = []
    for (cell, axis), total in zip(blocks, pushed):
        _, _, vector, index = other_of(cell, axis)
        if axis is not None and cell[axis] + 1 == local[axis]:
            remote.append((vector, index, total))
            continue
        weight = 1.0 if axis is None else 2.0
        for which in range(3):
            own_pairs += weight * total[which] * row(vector, index, which)

    for axis in range(3):
        if sizes[axis] > 1:
            pl.when(exists(axis, 1))(lambda a=axis: next_copy(a, 1).wait_recv())

    for vector, index, total in remote:
        for which in range(3):
            own_pairs += 2.0 * total[which] * row(vector, index, which)
    cross_two = wall_sq + jnp.sum(own_pairs, axis=0, keepdims=True)

    sublane = lax.broadcasted_iota(jnp.int32, (lanes, width), 0)
    tile = jnp.where(sublane == 0, noise_sq, 0.0)
    for which, part in enumerate((cross_one, image_sq, cross_two)):
        tile = jnp.where(sublane == which + 1, part, tile)
    reduced = jnp.broadcast_to(jnp.sum(tile, axis=1, keepdims=True), (lanes, width))
    chosen = sublane == lax.broadcasted_iota(jnp.int32, (lanes, width), 1)
    partial = jnp.sum(jnp.where(chosen, reduced, 0.0), axis=0, keepdims=True)

    base = 0
    for number, stage in enumerate(offsets):
        count = len(stage)
        if count == 0:
            continue
        position = {offset: base + order for order, offset in enumerate(stage)}
        own = base + count
        sums[pl.ds(own, 1)] = partial
        copies = []
        for offset in stage:
            back = tuple((sizes[k] - offset[k]) % sizes[k] for k in range(3))
            copy = pltpu.make_async_remote_copy(
                src_ref=sums.at[pl.ds(own, 1)],
                dst_ref=sums.at[pl.ds(position[back], 1)],
                send_sem=send_sum.at[position[offset]],
                recv_sem=recv_sum.at[position[back]],
                device_id=shifted(here, sizes, offset),
                device_id_type=pl.DeviceIdType.MESH,
            )
            copy.start()
            copies.append((offset, copy))
        for offset, _ in copies:
            pltpu.make_async_remote_copy(
                src_ref=sums.at[pl.ds(own, 1)],
                dst_ref=sums.at[pl.ds(position[offset], 1)],
                send_sem=send_sum.at[position[offset]],
                recv_sem=recv_sum.at[position[offset]],
                device_id=shifted(here, sizes, offset),
                device_id_type=pl.DeviceIdType.MESH,
            ).wait_recv()
        partial = jnp.sum(sums[pl.ds(base, count + 1)], axis=0, keepdims=True)
        for _, copy in copies:
            copy.wait_send()
        base += -(-(count + 1) // lanes) * lanes

    def scalar(which):
        return jnp.sum(jnp.where(lane == which, partial, 0.0), axis=1, keepdims=True)

    noise, cross, image_norm, cross_next = (scalar(which) for which in range(4))
    alpha_one = cross / noise
    beta_sq = image_norm / noise - alpha_one * alpha_one
    alpha_two = (
        cross_next - 2.0 * alpha_one * image_norm + alpha_one * alpha_one * cross
    ) / (noise * beta_sq)
    root_det = jnp.sqrt(alpha_one * alpha_two - beta_sq)
    trace_root = jnp.sqrt(alpha_one + alpha_two + 2.0 * root_det)
    image_factor = 1.0 / trace_root
    noise_factor = root_det * image_factor
    for cell in cells:
        out_ref[cell] = (
            noise_factor * packed[cell + (pl.ds(3, 3),)]
            + image_factor * mapped[cell + (pl.ds(0, 3),)]
        )

    for axis, side in faces:
        pl.when(exists(axis, side))(lambda a=axis, s=side: halo_copy(a, s, False).wait_send())
    for axis in range(3):
        if sizes[axis] > 1:
            pl.when(exists(axis, 0))(lambda a=axis: next_copy(a, 0).wait_send())


def shards(sizes, positions, gaussian, counts):
    local, width = positions.shape[:3], positions.shape[-1]
    cells = local[0] * local[1] * local[2]
    f32 = jnp.float32
    vmem = lambda *shape: pltpu.VMEM(shape, f32)
    slabs = [tuple(1 if k == axis else local[k] for k in range(3)) for axis in range(3)]
    rows = sum(
        -(-(len(stage_offsets(sizes, axes)) + 1) // lanes) * lanes for axes in groups_of(sizes)
    )
    sem = lambda count: pltpu.SemaphoreType.DMA((count,))
    return pl.pallas_call(
        functools.partial(kernel, sizes, local, width),
        out_shape=jax.ShapeDtypeStruct(positions.shape, f32),
        in_specs=[
            pl.BlockSpec(memory_space=pltpu.SMEM),
            pl.BlockSpec(memory_space=pltpu.VMEM),
            pl.BlockSpec(memory_space=pltpu.VMEM),
        ],
        out_specs=pl.BlockSpec(memory_space=pltpu.VMEM),
        scratch_shapes=[
            vmem(*local, lanes, width),
            vmem(*local, lanes, width),
            *(vmem(2, *slab, lanes, width) for slab in slabs),
            *(vmem(*slab, lanes, width) for slab in slabs),
            vmem(*local, 3, width, width),
            vmem(*local, 3, width, width),
            vmem(*local, 3, width, width),
            vmem(4 * cells, width, width),
            vmem(4 * cells, width, width),
            vmem(rows, width),
            sem(6), sem(6), sem(3), sem(3), sem(rows), sem(rows),
        ],
        compiler_params=pltpu.CompilerParams(collective_id=0, has_side_effects=True),
    )(counts, positions, gaussian)


def solution(mesh):
    sizes = tuple(mesh.shape[name] for name in names)
    in_specs = (
        P("gx", "gy", "gz", None, None),
        P("gx", "gy", "gz", None, None),
        P("gx", "gy", "gz"),
    )
    out_specs = P("gx", "gy", "gz", None, None)
    return jax.shard_map(
        functools.partial(shards, sizes), mesh=mesh, in_specs=in_specs, out_specs=out_specs,
        check_vma=False,
    )
```

```python
import functools
import itertools

import jax
import jax.numpy as jnp
from jax import lax
from jax.experimental import pallas as pl
from jax.experimental.pallas import tpu as pltpu
from jax.sharding import PartitionSpec as P

wall_gap = 1.0
lanes = 8
direct_limit = 64
far_away = -4096.0
names = ("gx", "gy", "gz")


def groups_of(sizes):
    total = sizes[0] * sizes[1] * sizes[2]
    return [(0, 1, 2)] if total <= direct_limit else [(0,), (1,), (2,)]


def stage_offsets(sizes, axes):
    ranges = [range(sizes[k]) if k in axes else range(1) for k in range(3)]
    return [offset for offset in itertools.product(*ranges) if any(offset)]


def shifted(here, sizes, offset):
    return tuple(
        lax.rem(here[k] + offset[k], sizes[k]) if offset[k] else here[k] for k in range(3)
    )


def wall_mobility(height):
    inv_height = 1.0 / (height + wall_gap)
    squared = inv_height * inv_height
    cubed = squared * inv_height
    fourth = squared * squared
    fifth = fourth * inv_height
    eleventh = fifth * fifth * inv_height
    twelfth = eleventh * inv_height
    parallel = 1.0 - 0.5625 * inv_height + 0.125 * cubed - 0.17578125 * fourth - 0.0625 * fifth
    perpend = (
        1.0
        - 1.125 * inv_height
        + 0.5 * cubed
        - 0.57 * fourth
        + 0.2 * fifth
        + 0.035 * eleventh
        - 0.04 * twelfth
    )
    return parallel, parallel, perpend


def kernel(
    sizes, local, width, counts_hbm, pos_hbm, gauss_hbm, out_ref,
    counts_ref, pos_ref, gauss_ref, load_sem, packed, mapped, halo_x, halo_y, halo_z, next_x, next_y, next_z,
    column, image_column, acc, iso, dyad, sums,
    send_one, recv_one, send_two, recv_two, send_sum, recv_sum,
):
    here = tuple(lax.axis_index(name) for name in names)
    cells = list(itertools.product(*(range(size) for size in local)))
    halos, nexts = (halo_x, halo_y, halo_z), (next_x, next_y, next_z)
    stages = groups_of(sizes)
    offsets = [stage_offsets(sizes, axes) for axes in stages]
    faces = [(axis, side) for axis in range(3) if sizes[axis] > 1 for side in range(2)]
    groups = width // lanes

    def exists(axis, side):
        return here[axis] < sizes[axis] - 1 if side else here[axis] > 0

    def slab(axis, side):
        index = [slice(None)] * 3
        index[axis] = pl.ds(local[axis] - 1 if side else 0, 1)
        return tuple(index)

    def beside(axis, side):
        return {names[axis]: here[axis] + (1 if side else -1)}

    loads = [
        pltpu.make_async_copy(source, target, load_sem.at[order])
        for order, (source, target) in enumerate(
            ((pos_hbm, pos_ref), (gauss_hbm, gauss_ref), (counts_hbm, counts_ref))
        )
    ]
    for load in loads:
        load.start()

    zero_tile = jnp.zeros((lanes, width), jnp.float32)
    tile_row = lax.broadcasted_iota(jnp.int32, (lanes, width), 0)
    outside = jnp.where(tile_row < 3, far_away, 0.0)
    for axis in range(3):
        face_cells = [c for c in cells if c[axis] == 0]
        for side in range(2):
            def clear(axis=axis, side=side, face_cells=face_cells):
                for cell in face_cells:
                    halos[axis][(side,) + cell] = outside
                    if side:
                        nexts[axis][cell] = zero_tile
            pl.when(jnp.logical_not(exists(axis, side)))(clear)

    barrier = pltpu.get_barrier_semaphore()
    peers = [offset for stage in offsets for offset in stage]
    for offset in peers:
        pl.semaphore_signal(
            barrier, inc=1, device_id=shifted(here, sizes, offset),
            device_id_type=pl.DeviceIdType.MESH,
        )

    for load in loads:
        load.wait()
    lane = lax.broadcasted_iota(jnp.int32, (1, width), 1)
    occupied, walls = {}, {}
    for cell in cells:
        occupied[cell] = (lane < counts_ref[cell]).astype(jnp.float32)
        for which in range(3):
            from_array = cell[:2] + (which, pl.ds(cell[2], 1))
            packed[cell + (pl.ds(which, 1),)] = pos_ref[from_array]
            packed[cell + (pl.ds(3 + which, 1),)] = gauss_ref[from_array] * occupied[cell]
        packed[cell + (pl.ds(6, 2),)] = jnp.zeros((2, width), jnp.float32)
        walls[cell] = wall_mobility(packed[cell + (pl.ds(2, 1),)])

    def row(ref, index, which):
        return ref[index + (pl.ds(which, 1),)]

    def spread(ref, cell, values):
        for which in range(3):
            full = jnp.broadcast_to(values[which], (width, width))
            ref[cell + (which,)] = full.T

    for cell in cells:
        spread(column, cell, [row(packed, cell, which) for which in range(3)])

    def source_of(cell, axis, side):
        there = list(cell)
        there[axis] += 1 if side else -1
        if 0 <= there[axis] < local[axis]:
            return packed, tuple(there), False
        there[axis] = 0
        return halos[axis], (side,) + tuple(there), True

    inner, outer, saved = {}, {}, []
    for cell in cells:
        inner[cell] = [(packed, cell, None)]
        outer[cell] = []
        saved.append((cell, None))
        for axis in range(3):
            for side in range(2):
                ref, index, remote = source_of(cell, axis, side)
                if remote and sizes[axis] == 1:
                    continue
                (outer if remote else inner)[cell].append((ref, index, (axis, side)))
                if side:
                    saved.append((cell, axis))
    slot_of = {key: slot for slot, key in enumerate(saved)}

    def diagonal(group):
        rows = group * lanes + lax.broadcasted_iota(jnp.int32, (lanes, width), 0)
        return rows == lax.broadcasted_iota(jnp.int32, (lanes, width), 1)

    def first_product(table, start):
        def body(group, carry):
            rows = pl.ds(pl.multiple_of(group * lanes, lanes), lanes)
            for cell in cells:
                target = [column[cell + (which, rows)] for which in range(3)]
                total = None if start else [acc[cell + (which, rows)] for which in range(3)]
                for ref, index, direction in table[cell]:
                    delta = [target[which] - row(ref, index, which) for which in range(3)]
                    value = [row(ref, index, 3 + which) for which in range(3)]
                    square = delta[0] * delta[0] + delta[1] * delta[1] + delta[2] * delta[2]
                    inverse = lax.rsqrt(square)
                    if direction is None:
                        inverse = jnp.where(diagonal(group), 0.0, inverse)
                    inv_sq = inverse * inverse
                    isotropic = inverse * (0.75 + 0.5 * inv_sq)
                    dyadic = (inverse * inv_sq) * (0.75 - 1.5 * inv_sq)
                    if direction is None or direction[1]:
                        slot = slot_of[(cell, None if direction is None else direction[0])]
                        iso[slot, rows] = isotropic
                        dyad[slot, rows] = dyadic
                    scaled = dyadic * (
                        delta[0] * value[0] + delta[1] * value[1] + delta[2] * value[2]
                    )
                    part = [isotropic * value[which] + delta[which] * scaled for which in range(3)]
                    total = part if total is None else [a + b for a, b in zip(total, part)]
                for which in range(3):
                    acc[cell + (which, rows)] = total[which]
            return carry

        lax.fori_loop(0, groups, body, 0)

    first_product(inner, True)

    pl.semaphore_wait(barrier, len(peers))

    def halo_copy(axis, side, receiver):
        held = side if receiver else 1 - side
        face = 2 * axis + held
        return pltpu.make_async_remote_copy(
            src_ref=packed.at[slab(axis, side)],
            dst_ref=halos[axis].at[held],
            send_sem=send_one.at[2 * axis + side],
            recv_sem=recv_one.at[face],
            device_id=beside(axis, side),
            device_id_type=pl.DeviceIdType.MESH,
        )

    def next_copy(axis, side):
        return pltpu.make_async_remote_copy(
            src_ref=mapped.at[slab(axis, 0)],
            dst_ref=nexts[axis],
            send_sem=send_two.at[axis],
            recv_sem=recv_two.at[axis],
            device_id=beside(axis, side),
            device_id_type=pl.DeviceIdType.MESH,
        )

    for axis, side in faces:
        pl.when(exists(axis, side))(lambda a=axis, s=side: halo_copy(a, s, False).start())
    for axis, side in faces:
        pl.when(exists(axis, side))(lambda a=axis, s=side: halo_copy(a, s, True).wait_recv())

    first_product(outer, False)

    images = {}
    for cell in cells:
        images[cell] = []
        for which in range(3):
            summed = jnp.sum(acc[cell + (which,)].T, axis=0, keepdims=True)
            value = row(packed, cell, 3 + which)
            image = (walls[cell][which] * value + summed) * occupied[cell]
            images[cell].append(image)
            mapped[cell + (pl.ds(which, 1),)] = image
        mapped[cell + (pl.ds(3, lanes - 3),)] = jnp.zeros((lanes - 3, width), jnp.float32)

    for axis in range(3):
        if sizes[axis] > 1:
            pl.when(exists(axis, 0))(lambda a=axis: next_copy(a, 0).start())

    for cell in cells:
        spread(image_column, cell, images[cell])

    def other_of(cell, axis):
        there = list(cell)
        if axis is None:
            return packed, cell, mapped, cell
        there[axis] += 1
        if there[axis] < local[axis]:
            return packed, tuple(there), mapped, tuple(there)
        there[axis] = 0
        return halos[axis], (1,) + tuple(there), nexts[axis], tuple(there)

    blocks = [
        key for key in saved
        if key[1] is None or key[0][key[1]] + 1 < local[key[1]] or sizes[key[1]] > 1
    ]

    def second_body(group, carry):
        rows = pl.ds(pl.multiple_of(group * lanes, lanes), lanes)
        result = []
        for (cell, axis), total in zip(blocks, carry):
            place, index, _, _ = other_of(cell, axis)
            slot = slot_of[(cell, axis)]
            delta = [
                column[cell + (which, rows)] - row(place, index, which) for which in range(3)
            ]
            value = [image_column[cell + (which, rows)] for which in range(3)]
            isotropic = iso[slot, rows]
            scaled = dyad[slot, rows] * (
                delta[0] * value[0] + delta[1] * value[1] + delta[2] * value[2]
            )
            result.append(tuple(
                total[which] + isotropic * value[which] + delta[which] * scaled
                for which in range(3)
            ))
        return tuple(result)

    zero = (jnp.zeros((lanes, width), jnp.float32),) * 3
    pushed = lax.fori_loop(0, groups, second_body, (zero,) * len(blocks))

    noise_sq = cross_one = image_sq = wall_sq = jnp.zeros((1, width), jnp.float32)
    for cell in cells:
        for which in range(3):
            value, image = row(packed, cell, 3 + which), images[cell][which]
            noise_sq += value * value
            cross_one += value * image
            image_sq += image * image
            wall_sq += walls[cell][which] * image * image

    own_pairs = jnp.zeros((lanes, width), jnp.float32)
    remote = []
    for (cell, axis), total in zip(blocks, pushed):
        _, _, vector, index = other_of(cell, axis)
        if axis is not None and cell[axis] + 1 == local[axis]:
            remote.append((vector, index, total))
            continue
        weight = 1.0 if axis is None else 2.0
        for which in range(3):
            own_pairs += weight * total[which] * row(vector, index, which)

    for axis in range(3):
        if sizes[axis] > 1:
            pl.when(exists(axis, 1))(lambda a=axis: next_copy(a, 1).wait_recv())

    for vector, index, total in remote:
        for which in range(3):
            own_pairs += 2.0 * total[which] * row(vector, index, which)
    cross_two = wall_sq + jnp.sum(own_pairs, axis=0, keepdims=True)

    sublane = lax.broadcasted_iota(jnp.int32, (lanes, width), 0)
    tile = jnp.where(sublane == 0, noise_sq, 0.0)
    for which, part in enumerate((cross_one, image_sq, cross_two)):
        tile = jnp.where(sublane == which + 1, part, tile)
    reduced = jnp.broadcast_to(jnp.sum(tile, axis=1, keepdims=True), (lanes, width))
    chosen = sublane == lax.broadcasted_iota(jnp.int32, (lanes, width), 1)
    partial = jnp.sum(jnp.where(chosen, reduced, 0.0), axis=0, keepdims=True)

    base = 0
    for number, stage in enumerate(offsets):
        count = len(stage)
        if count == 0:
            continue
        position = {offset: base + order for order, offset in enumerate(stage)}
        own = base + count
        sums[pl.ds(own, 1)] = partial
        copies = []
        for offset in stage:
            back = tuple((sizes[k] - offset[k]) % sizes[k] for k in range(3))
            copy = pltpu.make_async_remote_copy(
                src_ref=sums.at[pl.ds(own, 1)],
                dst_ref=sums.at[pl.ds(position[back], 1)],
                send_sem=send_sum.at[position[offset]],
                recv_sem=recv_sum.at[position[back]],
                device_id=shifted(here, sizes, offset),
                device_id_type=pl.DeviceIdType.MESH,
            )
            copy.start()
            copies.append((offset, copy))
        for offset, _ in copies:
            pltpu.make_async_remote_copy(
                src_ref=sums.at[pl.ds(own, 1)],
                dst_ref=sums.at[pl.ds(position[offset], 1)],
                send_sem=send_sum.at[position[offset]],
                recv_sem=recv_sum.at[position[offset]],
                device_id=shifted(here, sizes, offset),
                device_id_type=pl.DeviceIdType.MESH,
            ).wait_recv()
        partial = jnp.sum(sums[pl.ds(base, count + 1)], axis=0, keepdims=True)
        for _, copy in copies:
            copy.wait_send()
        base += -(-(count + 1) // lanes) * lanes

    def scalar(which):
        return jnp.sum(jnp.where(lane == which, partial, 0.0), axis=1, keepdims=True)

    noise, cross, image_norm, cross_next = (scalar(which) for which in range(4))
    alpha_one = cross / noise
    beta_sq = image_norm / noise - alpha_one * alpha_one
    alpha_two = (
        cross_next - 2.0 * alpha_one * image_norm + alpha_one * alpha_one * cross
    ) / (noise * beta_sq)
    root_det = jnp.sqrt(alpha_one * alpha_two - beta_sq)
    trace_root = jnp.sqrt(alpha_one + alpha_two + 2.0 * root_det)
    image_factor = 1.0 / trace_root
    noise_factor = root_det * image_factor
    for cell in cells:
        for which in range(3):
            out_ref[cell[:2] + (which, pl.ds(cell[2], 1))] = (
                noise_factor * row(packed, cell, 3 + which)
                + image_factor * row(mapped, cell, which)
            )

    for axis, side in faces:
        pl.when(exists(axis, side))(lambda a=axis, s=side: halo_copy(a, s, False).wait_send())
    for axis in range(3):
        if sizes[axis] > 1:
            pl.when(exists(axis, 0))(lambda a=axis: next_copy(a, 0).wait_send())


def shards(sizes, positions, gaussian, counts):
    local, width = positions.shape[:3], positions.shape[-1]
    cells = local[0] * local[1] * local[2]
    f32 = jnp.float32
    vmem = lambda *shape: pltpu.VMEM(shape, f32)
    sem = lambda count: pltpu.SemaphoreType.DMA((count,))
    slabs = [tuple(1 if k == axis else local[k] for k in range(3)) for axis in range(3)]
    rows = sum(
        -(-(len(stage_offsets(sizes, axes)) + 1) // lanes) * lanes for axes in groups_of(sizes)
    )
    order = (0, 1, 3, 2, 4)
    positions, gaussian = (jnp.transpose(array, order) for array in (positions, gaussian))
    result = pl.pallas_call(
        functools.partial(kernel, sizes, local, width),
        out_shape=jax.ShapeDtypeStruct(positions.shape, f32),
        in_specs=[pl.BlockSpec(memory_space=pltpu.HBM)] * 3,
        out_specs=pl.BlockSpec(memory_space=pltpu.VMEM),
        scratch_shapes=[
            pltpu.SMEM(counts.shape, jnp.int32),
            vmem(*positions.shape),
            vmem(*positions.shape),
            sem(3),
            vmem(*local, lanes, width),
            vmem(*local, lanes, width),
            *(vmem(2, *slab, lanes, width) for slab in slabs),
            *(vmem(*slab, lanes, width) for slab in slabs),
            vmem(*local, 3, width, width),
            vmem(*local, 3, width, width),
            vmem(*local, 3, width, width),
            vmem(4 * cells, width, width),
            vmem(4 * cells, width, width),
            vmem(rows, width),
            sem(6), sem(6), sem(3), sem(3), sem(rows), sem(rows),
        ],
        compiler_params=pltpu.CompilerParams(collective_id=0, has_side_effects=True),
    )(counts, positions, gaussian)
    return jnp.transpose(result, order)


def solution(mesh):
    sizes = tuple(mesh.shape[name] for name in names)
    in_specs = (
        P("gx", "gy", "gz", None, None),
        P("gx", "gy", "gz", None, None),
        P("gx", "gy", "gz"),
    )
    out_specs = P("gx", "gy", "gz", None, None)
    return jax.shard_map(
        functools.partial(shards, sizes), mesh=mesh, in_specs=in_specs, out_specs=out_specs,
        check_vma=False,
    )
```

```python
import functools
import itertools

import jax
import jax.numpy as jnp
from jax import lax
from jax.experimental import pallas as pl
from jax.experimental.pallas import tpu as pltpu
from jax.sharding import PartitionSpec as P

wall_gap = 1.0
lanes = 8
direct_limit = 64
far_away = -4096.0
names = ("gx", "gy", "gz")


def groups_of(sizes):
    total = sizes[0] * sizes[1] * sizes[2]
    return [(0, 1, 2)] if total <= direct_limit else [(0,), (1,), (2,)]


def stage_offsets(sizes, axes):
    ranges = [range(sizes[k]) if k in axes else range(1) for k in range(3)]
    return [offset for offset in itertools.product(*ranges) if any(offset)]


def barrier_offsets(sizes):
    stages = groups_of(sizes)
    if len(stages) > 1:
        return [offset for axes in stages for offset in stage_offsets(sizes, axes)], []
    plane = stage_offsets(sizes, (0, 1))
    return plane + stage_offsets(sizes, (2,)), plane


def around(here, sizes):
    table = []
    for k in range(3):
        ahead = [here[k] + step for step in range(sizes[k])]
        table.append([jnp.where(at >= sizes[k], at - sizes[k], at) for at in ahead])
    return table


def wall_mobility(height):
    inv_height = 1.0 / (height + wall_gap)
    squared = inv_height * inv_height
    cubed = squared * inv_height
    fourth = squared * squared
    fifth = fourth * inv_height
    eleventh = fifth * fifth * inv_height
    twelfth = eleventh * inv_height
    parallel = 1.0 - 0.5625 * inv_height + 0.125 * cubed - 0.17578125 * fourth - 0.0625 * fifth
    perpend = (
        1.0
        - 1.125 * inv_height
        + 0.5 * cubed
        - 0.57 * fourth
        + 0.2 * fifth
        + 0.035 * eleventh
        - 0.04 * twelfth
    )
    return parallel, parallel, perpend


def kernel(
    sizes, local, width, counts_hbm, pos_hbm, gauss_hbm, out_ref,
    counts_ref, pos_ref, gauss_ref, load_sem, packed, mapped, halo_x, halo_y, halo_z, next_x, next_y, next_z,
    column, image_column, acc, iso, dyad, sums,
    send_one, recv_one, send_two, recv_two, send_sum, recv_sum, told_sem,
):
    here = tuple(lax.axis_index(name) for name in names)
    cells = list(itertools.product(*(range(size) for size in local)))
    halos, nexts = (halo_x, halo_y, halo_z), (next_x, next_y, next_z)
    stages = groups_of(sizes)
    offsets = [stage_offsets(sizes, axes) for axes in stages]
    faces = [(axis, side) for axis in range(3) if sizes[axis] > 1 for side in range(2)]
    groups = width // lanes

    def exists(axis, side):
        return here[axis] < sizes[axis] - 1 if side else here[axis] > 0

    def slab(axis, side):
        index = [slice(None)] * 3
        index[axis] = pl.ds(local[axis] - 1 if side else 0, 1)
        return tuple(index)

    def beside(axis, side):
        return {names[axis]: here[axis] + (1 if side else -1)}

    loads = [
        pltpu.make_async_copy(source, target, load_sem.at[order])
        for order, (source, target) in enumerate(
            ((pos_hbm, pos_ref), (gauss_hbm, gauss_ref), (counts_hbm, counts_ref))
        )
    ]
    for load in loads:
        load.start()

    ring = around(here, sizes)

    def shifted(offset):
        return tuple(ring[k][offset[k]] for k in range(3))

    barrier = pltpu.get_barrier_semaphore()
    peers, told = barrier_offsets(sizes)
    for offset in peers:
        pl.semaphore_signal(
            barrier, inc=1, device_id=shifted(offset),
            device_id_type=pl.DeviceIdType.MESH,
        )

    zero_tile = jnp.zeros((lanes, width), jnp.float32)
    tile_row = lax.broadcasted_iota(jnp.int32, (lanes, width), 0)
    outside = jnp.where(tile_row < 3, far_away, 0.0)
    for axis in range(3):
        face_cells = [c for c in cells if c[axis] == 0]
        for side in range(2):
            def clear(axis=axis, side=side, face_cells=face_cells):
                for cell in face_cells:
                    halos[axis][(side,) + cell] = outside
                    if side:
                        nexts[axis][cell] = zero_tile
            pl.when(jnp.logical_not(exists(axis, side)))(clear)

    for load in loads:
        load.wait()
    lane = lax.broadcasted_iota(jnp.int32, (1, width), 1)
    occupied, walls = {}, {}
    for cell in cells:
        occupied[cell] = (lane < counts_ref[cell]).astype(jnp.float32)
        for which in range(3):
            from_array = cell[:2] + (which, pl.ds(cell[2], 1))
            packed[cell + (pl.ds(which, 1),)] = pos_ref[from_array]
            packed[cell + (pl.ds(3 + which, 1),)] = gauss_ref[from_array] * occupied[cell]
        packed[cell + (pl.ds(6, 2),)] = jnp.zeros((2, width), jnp.float32)
        walls[cell] = wall_mobility(packed[cell + (pl.ds(2, 1),)])

    def row(ref, index, which):
        return ref[index + (pl.ds(which, 1),)]

    def spread(ref, cell, values):
        for which in range(3):
            full = jnp.broadcast_to(values[which], (width, width))
            ref[cell + (which,)] = full.T

    for cell in cells:
        spread(column, cell, [row(packed, cell, which) for which in range(3)])

    def source_of(cell, axis, side):
        there = list(cell)
        there[axis] += 1 if side else -1
        if 0 <= there[axis] < local[axis]:
            return packed, tuple(there), False
        there[axis] = 0
        return halos[axis], (side,) + tuple(there), True

    inner, outer, saved = {}, {}, []
    for cell in cells:
        inner[cell] = [(packed, cell, None)]
        outer[cell] = []
        saved.append((cell, None))
        for axis in range(3):
            for side in range(2):
                ref, index, remote = source_of(cell, axis, side)
                if remote and sizes[axis] == 1:
                    continue
                (outer if remote else inner)[cell].append((ref, index, (axis, side)))
                if side:
                    saved.append((cell, axis))
    slot_of = {key: slot for slot, key in enumerate(saved)}

    def diagonal(group):
        rows = group * lanes + lax.broadcasted_iota(jnp.int32, (lanes, width), 0)
        return rows == lax.broadcasted_iota(jnp.int32, (lanes, width), 1)

    def first_product(table, start):
        def body(group, carry):
            rows = pl.ds(pl.multiple_of(group * lanes, lanes), lanes)
            for cell in cells:
                target = [column[cell + (which, rows)] for which in range(3)]
                total = None if start else [acc[cell + (which, rows)] for which in range(3)]
                for ref, index, direction in table[cell]:
                    delta = [target[which] - row(ref, index, which) for which in range(3)]
                    value = [row(ref, index, 3 + which) for which in range(3)]
                    square = delta[0] * delta[0] + delta[1] * delta[1] + delta[2] * delta[2]
                    inverse = lax.rsqrt(square)
                    if direction is None:
                        inverse = jnp.where(diagonal(group), 0.0, inverse)
                    inv_sq = inverse * inverse
                    isotropic = inverse * (0.75 + 0.5 * inv_sq)
                    dyadic = (inverse * inv_sq) * (0.75 - 1.5 * inv_sq)
                    if direction is None or direction[1]:
                        slot = slot_of[(cell, None if direction is None else direction[0])]
                        iso[slot, rows] = isotropic
                        dyad[slot, rows] = dyadic
                    scaled = dyadic * (
                        delta[0] * value[0] + delta[1] * value[1] + delta[2] * value[2]
                    )
                    part = [isotropic * value[which] + delta[which] * scaled for which in range(3)]
                    total = part if total is None else [a + b for a, b in zip(total, part)]
                for which in range(3):
                    acc[cell + (which, rows)] = total[which]
            return carry

        lax.fori_loop(0, groups, body, 0)

    first_product(inner, True)

    pl.semaphore_wait(barrier, len(peers))

    def halo_copy(axis, side, receiver):
        held = side if receiver else 1 - side
        face = 2 * axis + held
        return pltpu.make_async_remote_copy(
            src_ref=packed.at[slab(axis, side)],
            dst_ref=halos[axis].at[held],
            send_sem=send_one.at[2 * axis + side],
            recv_sem=recv_one.at[face],
            device_id=beside(axis, side),
            device_id_type=pl.DeviceIdType.MESH,
        )

    def next_copy(axis, side):
        return pltpu.make_async_remote_copy(
            src_ref=mapped.at[slab(axis, 0)],
            dst_ref=nexts[axis],
            send_sem=send_two.at[axis],
            recv_sem=recv_two.at[axis],
            device_id=beside(axis, side),
            device_id_type=pl.DeviceIdType.MESH,
        )

    for axis, side in faces:
        pl.when(exists(axis, side))(lambda a=axis, s=side: halo_copy(a, s, False).start())
    for offset in told:
        pl.semaphore_signal(
            told_sem, inc=1, device_id=shifted(offset), device_id_type=pl.DeviceIdType.MESH
        )
    for axis, side in faces:
        pl.when(exists(axis, side))(lambda a=axis, s=side: halo_copy(a, s, True).wait_recv())

    first_product(outer, False)

    images = {}
    for cell in cells:
        images[cell] = []
        for which in range(3):
            summed = jnp.sum(acc[cell + (which,)].T, axis=0, keepdims=True)
            value = row(packed, cell, 3 + which)
            image = (walls[cell][which] * value + summed) * occupied[cell]
            images[cell].append(image)
            mapped[cell + (pl.ds(which, 1),)] = image
        mapped[cell + (pl.ds(3, lanes - 3),)] = jnp.zeros((lanes - 3, width), jnp.float32)

    for axis in range(3):
        if sizes[axis] > 1:
            pl.when(exists(axis, 0))(lambda a=axis: next_copy(a, 0).start())

    for cell in cells:
        spread(image_column, cell, images[cell])

    def other_of(cell, axis):
        there = list(cell)
        if axis is None:
            return packed, cell, mapped, cell
        there[axis] += 1
        if there[axis] < local[axis]:
            return packed, tuple(there), mapped, tuple(there)
        there[axis] = 0
        return halos[axis], (1,) + tuple(there), nexts[axis], tuple(there)

    blocks = [
        key for key in saved
        if key[1] is None or key[0][key[1]] + 1 < local[key[1]] or sizes[key[1]] > 1
    ]

    def second_body(group, carry):
        rows = pl.ds(pl.multiple_of(group * lanes, lanes), lanes)
        result = []
        for (cell, axis), total in zip(blocks, carry):
            place, index, _, _ = other_of(cell, axis)
            slot = slot_of[(cell, axis)]
            delta = [
                column[cell + (which, rows)] - row(place, index, which) for which in range(3)
            ]
            value = [image_column[cell + (which, rows)] for which in range(3)]
            isotropic = iso[slot, rows]
            scaled = dyad[slot, rows] * (
                delta[0] * value[0] + delta[1] * value[1] + delta[2] * value[2]
            )
            result.append(tuple(
                total[which] + isotropic * value[which] + delta[which] * scaled
                for which in range(3)
            ))
        return tuple(result)

    zero = (jnp.zeros((lanes, width), jnp.float32),) * 3
    pushed = lax.fori_loop(0, groups, second_body, (zero,) * len(blocks))

    noise_sq = cross_one = image_sq = wall_sq = jnp.zeros((1, width), jnp.float32)
    for cell in cells:
        for which in range(3):
            value, image = row(packed, cell, 3 + which), images[cell][which]
            noise_sq += value * value
            cross_one += value * image
            image_sq += image * image
            wall_sq += walls[cell][which] * image * image

    own_pairs = jnp.zeros((lanes, width), jnp.float32)
    remote = []
    for (cell, axis), total in zip(blocks, pushed):
        _, _, vector, index = other_of(cell, axis)
        if axis is not None and cell[axis] + 1 == local[axis]:
            remote.append((vector, index, total))
            continue
        weight = 1.0 if axis is None else 2.0
        for which in range(3):
            own_pairs += weight * total[which] * row(vector, index, which)

    for axis in range(3):
        if sizes[axis] > 1:
            pl.when(exists(axis, 1))(lambda a=axis: next_copy(a, 1).wait_recv())

    for vector, index, total in remote:
        for which in range(3):
            own_pairs += 2.0 * total[which] * row(vector, index, which)
    cross_two = wall_sq + jnp.sum(own_pairs, axis=0, keepdims=True)

    sublane = lax.broadcasted_iota(jnp.int32, (lanes, width), 0)
    tile = jnp.where(sublane == 0, noise_sq, 0.0)
    for which, part in enumerate((cross_one, image_sq, cross_two)):
        tile = jnp.where(sublane == which + 1, part, tile)
    reduced = jnp.broadcast_to(jnp.sum(tile, axis=1, keepdims=True), (lanes, width))
    chosen = sublane == lax.broadcasted_iota(jnp.int32, (lanes, width), 1)
    partial = jnp.sum(jnp.where(chosen, reduced, 0.0), axis=0, keepdims=True)

    if told:
        pl.semaphore_wait(told_sem, len(told))
    base = 0
    for number, stage in enumerate(offsets):
        count = len(stage)
        if count == 0:
            continue
        position = {offset: base + order for order, offset in enumerate(stage)}
        own = base + count
        sums[pl.ds(own, 1)] = partial
        copies = []
        for offset in stage:
            back = tuple((sizes[k] - offset[k]) % sizes[k] for k in range(3))
            copy = pltpu.make_async_remote_copy(
                src_ref=sums.at[pl.ds(own, 1)],
                dst_ref=sums.at[pl.ds(position[back], 1)],
                send_sem=send_sum.at[position[offset]],
                recv_sem=recv_sum.at[position[back]],
                device_id=shifted(offset),
                device_id_type=pl.DeviceIdType.MESH,
            )
            copy.start()
            copies.append((offset, copy))
        for offset, _ in copies:
            pltpu.make_async_remote_copy(
                src_ref=sums.at[pl.ds(own, 1)],
                dst_ref=sums.at[pl.ds(position[offset], 1)],
                send_sem=send_sum.at[position[offset]],
                recv_sem=recv_sum.at[position[offset]],
                device_id=shifted(offset),
                device_id_type=pl.DeviceIdType.MESH,
            ).wait_recv()
        partial = jnp.sum(sums[pl.ds(base, count + 1)], axis=0, keepdims=True)
        for _, copy in copies:
            copy.wait_send()
        base += -(-(count + 1) // lanes) * lanes

    def scalar(which):
        return jnp.sum(jnp.where(lane == which, partial, 0.0), axis=1, keepdims=True)

    noise, cross, image_norm, cross_next = (scalar(which) for which in range(4))
    alpha_one = cross / noise
    beta_sq = image_norm / noise - alpha_one * alpha_one
    alpha_two = (
        cross_next - 2.0 * alpha_one * image_norm + alpha_one * alpha_one * cross
    ) / (noise * beta_sq)
    root_det = jnp.sqrt(alpha_one * alpha_two - beta_sq)
    trace_root = jnp.sqrt(alpha_one + alpha_two + 2.0 * root_det)
    image_factor = 1.0 / trace_root
    noise_factor = root_det * image_factor
    for cell in cells:
        for which in range(3):
            out_ref[cell[:2] + (which, pl.ds(cell[2], 1))] = (
                noise_factor * row(packed, cell, 3 + which)
                + image_factor * row(mapped, cell, which)
            )

    for axis, side in faces:
        pl.when(exists(axis, side))(lambda a=axis, s=side: halo_copy(a, s, False).wait_send())
    for axis in range(3):
        if sizes[axis] > 1:
            pl.when(exists(axis, 0))(lambda a=axis: next_copy(a, 0).wait_send())


def shards(sizes, positions, gaussian, counts):
    local, width = positions.shape[:3], positions.shape[-1]
    cells = local[0] * local[1] * local[2]
    f32 = jnp.float32
    vmem = lambda *shape: pltpu.VMEM(shape, f32)
    sem = lambda count: pltpu.SemaphoreType.DMA((count,))
    slabs = [tuple(1 if k == axis else local[k] for k in range(3)) for axis in range(3)]
    rows = sum(
        -(-(len(stage_offsets(sizes, axes)) + 1) // lanes) * lanes for axes in groups_of(sizes)
    )
    order = (0, 1, 3, 2, 4)
    positions, gaussian = (jnp.transpose(array, order) for array in (positions, gaussian))
    result = pl.pallas_call(
        functools.partial(kernel, sizes, local, width),
        out_shape=pltpu.VMEM(positions.shape, f32),
        in_specs=[pl.BlockSpec(memory_space=pltpu.HBM)] * 3,
        out_specs=pl.BlockSpec(memory_space=pltpu.VMEM),
        scratch_shapes=[
            pltpu.SMEM(counts.shape, jnp.int32),
            vmem(*positions.shape),
            vmem(*positions.shape),
            sem(3),
            vmem(*local, lanes, width),
            vmem(*local, lanes, width),
            *(vmem(2, *slab, lanes, width) for slab in slabs),
            *(vmem(*slab, lanes, width) for slab in slabs),
            vmem(*local, 3, width, width),
            vmem(*local, 3, width, width),
            vmem(*local, 3, width, width),
            vmem(4 * cells, width, width),
            vmem(4 * cells, width, width),
            vmem(rows, width),
            sem(6), sem(6), sem(3), sem(3), sem(rows), sem(rows), pltpu.SemaphoreType.REGULAR,
        ],
        compiler_params=pltpu.CompilerParams(collective_id=0, has_side_effects=True),
    )(counts, positions, gaussian)
    return jnp.transpose(result, order)


def solution(mesh):
    sizes = tuple(mesh.shape[name] for name in names)
    in_specs = (
        P("gx", "gy", "gz", None, None),
        P("gx", "gy", "gz", None, None),
        P("gx", "gy", "gz"),
    )
    out_specs = P("gx", "gy", "gz", None, None)
    return jax.shard_map(
        functools.partial(shards, sizes), mesh=mesh, in_specs=in_specs, out_specs=out_specs,
        check_vma=False,
    )
```

```python
import functools
import itertools

import jax
import jax.numpy as jnp
from jax import lax
from jax.experimental import pallas as pl
from jax.experimental.pallas import tpu as pltpu
from jax.sharding import PartitionSpec as P

wall_gap = 1.0
lanes = 8
direct_limit = 64
far_away = -4096.0
names = ("gx", "gy", "gz")


def groups_of(sizes):
    total = sizes[0] * sizes[1] * sizes[2]
    return [(0, 1, 2)] if total <= direct_limit else [(0,), (1,), (2,)]


def stage_offsets(sizes, axes):
    ranges = [range(sizes[k]) if k in axes else range(1) for k in range(3)]
    away = lambda offset: sum(min(o, size - o) for o, size in zip(offset, sizes))
    found = [offset for offset in itertools.product(*ranges) if any(offset)]
    return sorted(found, key=away, reverse=True)


def barrier_offsets(sizes):
    stages = groups_of(sizes)
    if len(stages) > 1:
        return [offset for axes in stages for offset in stage_offsets(sizes, axes)], []
    plane = stage_offsets(sizes, (0, 1))
    return plane + stage_offsets(sizes, (2,)), plane


def around(here, sizes):
    table = []
    for k in range(3):
        ahead = [here[k] + step for step in range(sizes[k])]
        table.append([jnp.where(at >= sizes[k], at - sizes[k], at) for at in ahead])
    return table


def wall_mobility(height):
    inv_height = 1.0 / (height + wall_gap)
    squared = inv_height * inv_height
    cubed = squared * inv_height
    fourth = squared * squared
    fifth = fourth * inv_height
    eleventh = fifth * fifth * inv_height
    twelfth = eleventh * inv_height
    parallel = 1.0 - 0.5625 * inv_height + 0.125 * cubed - 0.17578125 * fourth - 0.0625 * fifth
    perpend = (
        1.0
        - 1.125 * inv_height
        + 0.5 * cubed
        - 0.57 * fourth
        + 0.2 * fifth
        + 0.035 * eleventh
        - 0.04 * twelfth
    )
    return parallel, parallel, perpend


def kernel(
    sizes, local, width, counts_hbm, pos_hbm, gauss_hbm, out_ref,
    counts_ref, pos_ref, gauss_ref, load_sem, packed, mapped, halo_x, halo_y, halo_z, next_x, next_y, next_z,
    column, image_column, acc, iso, dyad, sums,
    send_one, recv_one, send_two, recv_two, send_sum, recv_sum, told_sem,
):
    here = tuple(lax.axis_index(name) for name in names)
    cells = list(itertools.product(*(range(size) for size in local)))
    halos, nexts = (halo_x, halo_y, halo_z), (next_x, next_y, next_z)
    stages = groups_of(sizes)
    offsets = [stage_offsets(sizes, axes) for axes in stages]
    faces = [(axis, side) for axis in range(3) if sizes[axis] > 1 for side in range(2)]
    groups = width // lanes

    def exists(axis, side):
        return here[axis] < sizes[axis] - 1 if side else here[axis] > 0

    def slab(axis, side):
        index = [slice(None)] * 3
        index[axis] = pl.ds(local[axis] - 1 if side else 0, 1)
        return tuple(index)

    def beside(axis, side):
        return {names[axis]: here[axis] + (1 if side else -1)}

    loads = [
        pltpu.make_async_copy(source, target, load_sem.at[order])
        for order, (source, target) in enumerate(
            ((pos_hbm, pos_ref), (gauss_hbm, gauss_ref), (counts_hbm, counts_ref))
        )
    ]
    for load in loads:
        load.start()

    ring = around(here, sizes)

    def shifted(offset):
        return tuple(ring[k][offset[k]] for k in range(3))

    barrier = pltpu.get_barrier_semaphore()
    peers, told = barrier_offsets(sizes)
    for offset in peers:
        pl.semaphore_signal(
            barrier, inc=1, device_id=shifted(offset),
            device_id_type=pl.DeviceIdType.MESH,
        )

    zero_tile = jnp.zeros((lanes, width), jnp.float32)
    tile_row = lax.broadcasted_iota(jnp.int32, (lanes, width), 0)
    outside = jnp.where(tile_row < 3, far_away, 0.0)
    for axis in range(3):
        face_cells = [c for c in cells if c[axis] == 0]
        for side in range(2):
            def clear(axis=axis, side=side, face_cells=face_cells):
                for cell in face_cells:
                    halos[axis][(side,) + cell] = outside
                    if side:
                        nexts[axis][cell] = zero_tile
            pl.when(jnp.logical_not(exists(axis, side)))(clear)

    for load in loads:
        load.wait()
    lane = lax.broadcasted_iota(jnp.int32, (1, width), 1)
    occupied, walls = {}, {}
    for cell in cells:
        occupied[cell] = (lane < counts_ref[cell]).astype(jnp.float32)
        for which in range(3):
            from_array = cell[:2] + (which, pl.ds(cell[2], 1))
            packed[cell + (pl.ds(which, 1),)] = pos_ref[from_array]
            packed[cell + (pl.ds(3 + which, 1),)] = gauss_ref[from_array] * occupied[cell]
        packed[cell + (pl.ds(6, 2),)] = jnp.zeros((2, width), jnp.float32)
        walls[cell] = wall_mobility(packed[cell + (pl.ds(2, 1),)])

    def row(ref, index, which):
        return ref[index + (pl.ds(which, 1),)]

    def spread(ref, cell, values):
        for which in range(3):
            full = jnp.broadcast_to(values[which], (width, width))
            ref[cell + (which,)] = full.T

    def source_of(cell, axis, side):
        there = list(cell)
        there[axis] += 1 if side else -1
        if 0 <= there[axis] < local[axis]:
            return packed, tuple(there), False
        there[axis] = 0
        return halos[axis], (side,) + tuple(there), True

    inner, outer, saved = {}, {}, []
    for cell in cells:
        inner[cell] = [(packed, cell, None)]
        outer[cell] = []
        saved.append((cell, None))
        for axis in range(3):
            for side in range(2):
                ref, index, remote = source_of(cell, axis, side)
                if remote and sizes[axis] == 1:
                    continue
                (outer if remote else inner)[cell].append((ref, index, (axis, side)))
                if side:
                    saved.append((cell, axis))
    slot_of = {key: slot for slot, key in enumerate(saved)}

    def diagonal(group):
        rows = group * lanes + lax.broadcasted_iota(jnp.int32, (lanes, width), 0)
        return rows == lax.broadcasted_iota(jnp.int32, (lanes, width), 1)

    def first_product(table, start):
        def body(group, carry):
            rows = pl.ds(pl.multiple_of(group * lanes, lanes), lanes)
            for cell in cells:
                target = [column[cell + (which, rows)] for which in range(3)]
                total = None if start else [acc[cell + (which, rows)] for which in range(3)]
                for ref, index, direction in table[cell]:
                    delta = [target[which] - row(ref, index, which) for which in range(3)]
                    value = [row(ref, index, 3 + which) for which in range(3)]
                    square = delta[0] * delta[0] + delta[1] * delta[1] + delta[2] * delta[2]
                    inverse = lax.rsqrt(square)
                    if direction is None:
                        inverse = jnp.where(diagonal(group), 0.0, inverse)
                    inv_sq = inverse * inverse
                    isotropic = inverse * (0.75 + 0.5 * inv_sq)
                    dyadic = (inverse * inv_sq) * (0.75 - 1.5 * inv_sq)
                    if direction is None or direction[1]:
                        slot = slot_of[(cell, None if direction is None else direction[0])]
                        iso[slot, rows] = isotropic
                        dyad[slot, rows] = dyadic
                    scaled = dyadic * (
                        delta[0] * value[0] + delta[1] * value[1] + delta[2] * value[2]
                    )
                    part = [isotropic * value[which] + delta[which] * scaled for which in range(3)]
                    total = part if total is None else [a + b for a, b in zip(total, part)]
                for which in range(3):
                    acc[cell + (which, rows)] = total[which]
            return carry

        lax.fori_loop(0, groups, body, 0)

    pl.semaphore_wait(barrier, len(peers))

    def halo_copy(axis, side, receiver):
        held = side if receiver else 1 - side
        face = 2 * axis + held
        return pltpu.make_async_remote_copy(
            src_ref=packed.at[slab(axis, side)],
            dst_ref=halos[axis].at[held],
            send_sem=send_one.at[2 * axis + side],
            recv_sem=recv_one.at[face],
            device_id=beside(axis, side),
            device_id_type=pl.DeviceIdType.MESH,
        )

    def next_copy(axis, side):
        return pltpu.make_async_remote_copy(
            src_ref=mapped.at[slab(axis, 0)],
            dst_ref=nexts[axis],
            send_sem=send_two.at[axis],
            recv_sem=recv_two.at[axis],
            device_id=beside(axis, side),
            device_id_type=pl.DeviceIdType.MESH,
        )

    for axis, side in faces:
        pl.when(exists(axis, side))(lambda a=axis, s=side: halo_copy(a, s, False).start())
    for offset in told:
        pl.semaphore_signal(
            told_sem, inc=1, device_id=shifted(offset), device_id_type=pl.DeviceIdType.MESH
        )
    for cell in cells:
        spread(column, cell, [row(packed, cell, which) for which in range(3)])

    first_product(inner, True)

    for axis, side in faces:
        pl.when(exists(axis, side))(lambda a=axis, s=side: halo_copy(a, s, True).wait_recv())

    first_product(outer, False)

    images = {}
    for cell in cells:
        images[cell] = []
        for which in range(3):
            summed = jnp.sum(acc[cell + (which,)].T, axis=0, keepdims=True)
            value = row(packed, cell, 3 + which)
            image = (walls[cell][which] * value + summed) * occupied[cell]
            images[cell].append(image)
            mapped[cell + (pl.ds(which, 1),)] = image
        mapped[cell + (pl.ds(3, lanes - 3),)] = jnp.zeros((lanes - 3, width), jnp.float32)

    for axis in range(3):
        if sizes[axis] > 1:
            pl.when(exists(axis, 0))(lambda a=axis: next_copy(a, 0).start())

    for cell in cells:
        spread(image_column, cell, images[cell])

    def other_of(cell, axis):
        there = list(cell)
        if axis is None:
            return packed, cell, mapped, cell
        there[axis] += 1
        if there[axis] < local[axis]:
            return packed, tuple(there), mapped, tuple(there)
        there[axis] = 0
        return halos[axis], (1,) + tuple(there), nexts[axis], tuple(there)

    blocks = [
        key for key in saved
        if key[1] is None or key[0][key[1]] + 1 < local[key[1]] or sizes[key[1]] > 1
    ]

    def second_body(group, carry):
        rows = pl.ds(pl.multiple_of(group * lanes, lanes), lanes)
        result = []
        for (cell, axis), total in zip(blocks, carry):
            place, index, _, _ = other_of(cell, axis)
            slot = slot_of[(cell, axis)]
            delta = [
                column[cell + (which, rows)] - row(place, index, which) for which in range(3)
            ]
            value = [image_column[cell + (which, rows)] for which in range(3)]
            isotropic = iso[slot, rows]
            scaled = dyad[slot, rows] * (
                delta[0] * value[0] + delta[1] * value[1] + delta[2] * value[2]
            )
            result.append(tuple(
                total[which] + isotropic * value[which] + delta[which] * scaled
                for which in range(3)
            ))
        return tuple(result)

    zero = (jnp.zeros((lanes, width), jnp.float32),) * 3
    pushed = lax.fori_loop(0, groups, second_body, (zero,) * len(blocks))

    noise_sq = cross_one = image_sq = wall_sq = jnp.zeros((1, width), jnp.float32)
    for cell in cells:
        for which in range(3):
            value, image = row(packed, cell, 3 + which), images[cell][which]
            noise_sq += value * value
            cross_one += value * image
            image_sq += image * image
            wall_sq += walls[cell][which] * image * image

    own_pairs = jnp.zeros((lanes, width), jnp.float32)
    remote = []
    for (cell, axis), total in zip(blocks, pushed):
        _, _, vector, index = other_of(cell, axis)
        if axis is not None and cell[axis] + 1 == local[axis]:
            remote.append((vector, index, total))
            continue
        weight = 1.0 if axis is None else 2.0
        for which in range(3):
            own_pairs += weight * total[which] * row(vector, index, which)

    for axis in range(3):
        if sizes[axis] > 1:
            pl.when(exists(axis, 1))(lambda a=axis: next_copy(a, 1).wait_recv())

    for vector, index, total in remote:
        for which in range(3):
            own_pairs += 2.0 * total[which] * row(vector, index, which)
    cross_two = wall_sq + jnp.sum(own_pairs, axis=0, keepdims=True)

    sublane = lax.broadcasted_iota(jnp.int32, (lanes, width), 0)
    tile = jnp.where(sublane == 0, noise_sq, 0.0)
    for which, part in enumerate((cross_one, image_sq, cross_two)):
        tile = jnp.where(sublane == which + 1, part, tile)
    reduced = jnp.broadcast_to(jnp.sum(tile, axis=1, keepdims=True), (lanes, width))
    chosen = sublane == lax.broadcasted_iota(jnp.int32, (lanes, width), 1)
    partial = jnp.sum(jnp.where(chosen, reduced, 0.0), axis=0, keepdims=True)

    if told:
        pl.semaphore_wait(told_sem, len(told))
    base = 0
    for number, stage in enumerate(offsets):
        count = len(stage)
        if count == 0:
            continue
        position = {offset: base + order for order, offset in enumerate(stage)}
        own = base + count
        sums[pl.ds(own, 1)] = partial
        copies = []
        for offset in stage:
            back = tuple((sizes[k] - offset[k]) % sizes[k] for k in range(3))
            copy = pltpu.make_async_remote_copy(
                src_ref=sums.at[pl.ds(own, 1)],
                dst_ref=sums.at[pl.ds(position[back], 1)],
                send_sem=send_sum.at[position[offset]],
                recv_sem=recv_sum.at[position[back]],
                device_id=shifted(offset),
                device_id_type=pl.DeviceIdType.MESH,
            )
            copy.start()
            copies.append((offset, copy))
        for offset, _ in copies:
            pltpu.make_async_remote_copy(
                src_ref=sums.at[pl.ds(own, 1)],
                dst_ref=sums.at[pl.ds(position[offset], 1)],
                send_sem=send_sum.at[position[offset]],
                recv_sem=recv_sum.at[position[offset]],
                device_id=shifted(offset),
                device_id_type=pl.DeviceIdType.MESH,
            ).wait_recv()
        partial = jnp.sum(sums[pl.ds(base, count + 1)], axis=0, keepdims=True)
        for _, copy in copies:
            copy.wait_send()
        base += -(-(count + 1) // lanes) * lanes

    def scalar(which):
        return jnp.sum(jnp.where(lane == which, partial, 0.0), axis=1, keepdims=True)

    noise, cross, image_norm, cross_next = (scalar(which) for which in range(4))
    alpha_one = cross / noise
    beta_sq = image_norm / noise - alpha_one * alpha_one
    alpha_two = (
        cross_next - 2.0 * alpha_one * image_norm + alpha_one * alpha_one * cross
    ) / (noise * beta_sq)
    root_det = jnp.sqrt(alpha_one * alpha_two - beta_sq)
    trace_root = jnp.sqrt(alpha_one + alpha_two + 2.0 * root_det)
    image_factor = 1.0 / trace_root
    noise_factor = root_det * image_factor
    for cell in cells:
        for which in range(3):
            out_ref[cell[:2] + (which, pl.ds(cell[2], 1))] = (
                noise_factor * row(packed, cell, 3 + which)
                + image_factor * row(mapped, cell, which)
            )

    for axis, side in faces:
        pl.when(exists(axis, side))(lambda a=axis, s=side: halo_copy(a, s, False).wait_send())
    for axis in range(3):
        if sizes[axis] > 1:
            pl.when(exists(axis, 0))(lambda a=axis: next_copy(a, 0).wait_send())


def shards(sizes, positions, gaussian, counts):
    local, width = positions.shape[:3], positions.shape[-1]
    cells = local[0] * local[1] * local[2]
    f32 = jnp.float32
    vmem = lambda *shape: pltpu.VMEM(shape, f32)
    sem = lambda count: pltpu.SemaphoreType.DMA((count,))
    slabs = [tuple(1 if k == axis else local[k] for k in range(3)) for axis in range(3)]
    rows = sum(
        -(-(len(stage_offsets(sizes, axes)) + 1) // lanes) * lanes for axes in groups_of(sizes)
    )
    order = (0, 1, 3, 2, 4)
    positions, gaussian = (jnp.transpose(array, order) for array in (positions, gaussian))
    result = pl.pallas_call(
        functools.partial(kernel, sizes, local, width),
        out_shape=pltpu.VMEM(positions.shape, f32),
        in_specs=[pl.BlockSpec(memory_space=pltpu.HBM)] * 3,
        out_specs=pl.BlockSpec(memory_space=pltpu.VMEM),
        scratch_shapes=[
            pltpu.SMEM(counts.shape, jnp.int32),
            vmem(*positions.shape),
            vmem(*positions.shape),
            sem(3),
            vmem(*local, lanes, width),
            vmem(*local, lanes, width),
            *(vmem(2, *slab, lanes, width) for slab in slabs),
            *(vmem(*slab, lanes, width) for slab in slabs),
            vmem(*local, 3, width, width),
            vmem(*local, 3, width, width),
            vmem(*local, 3, width, width),
            vmem(4 * cells, width, width),
            vmem(4 * cells, width, width),
            vmem(rows, width),
            sem(6), sem(6), sem(3), sem(3), sem(rows), sem(rows), pltpu.SemaphoreType.REGULAR,
        ],
        compiler_params=pltpu.CompilerParams(collective_id=0, has_side_effects=True),
    )(counts, positions, gaussian)
    return jnp.transpose(result, order)


def solution(mesh):
    sizes = tuple(mesh.shape[name] for name in names)
    in_specs = (
        P("gx", "gy", "gz", None, None),
        P("gx", "gy", "gz", None, None),
        P("gx", "gy", "gz"),
    )
    out_specs = P("gx", "gy", "gz", None, None)
    return jax.shard_map(
        functools.partial(shards, sizes), mesh=mesh, in_specs=in_specs, out_specs=out_specs,
        check_vma=False,
    )
```

```python
import functools
import itertools

import jax
import jax.numpy as jnp
from jax import lax
from jax.experimental import pallas as pl
from jax.experimental.pallas import tpu as pltpu
from jax.sharding import PartitionSpec as P

wall_gap = 1.0
lanes = 8
direct_limit = 64
far_away = -4096.0
names = ("gx", "gy", "gz")


def groups_of(sizes):
    total = sizes[0] * sizes[1] * sizes[2]
    return [(0, 1, 2)] if total <= direct_limit else [(0,), (1,), (2,)]


def stage_offsets(sizes, axes):
    ranges = [range(sizes[k]) if k in axes else range(1) for k in range(3)]
    away = lambda offset: sum(min(o, size - o) for o, size in zip(offset, sizes))
    found = [offset for offset in itertools.product(*ranges) if any(offset)]
    return sorted(found, key=away, reverse=True)


def entry_plan(sizes):
    stages = groups_of(sizes)
    if len(stages) > 1:
        return [offset for axes in stages for offset in stage_offsets(sizes, axes)], False, []
    near = 1 < sizes[2] <= 4
    lines = stage_offsets(sizes, (0,)) + stage_offsets(sizes, (1,))
    plane = stage_offsets(sizes, (0, 1))
    return (lines if near else plane + stage_offsets(sizes, (2,))), near, plane


def around(here, sizes):
    table = []
    for k in range(3):
        ahead = [here[k] + step for step in range(sizes[k])]
        table.append([jnp.where(at >= sizes[k], at - sizes[k], at) for at in ahead])
    return table


def wall_mobility(height):
    inv_height = 1.0 / (height + wall_gap)
    squared = inv_height * inv_height
    cubed = squared * inv_height
    fourth = squared * squared
    fifth = fourth * inv_height
    eleventh = fifth * fifth * inv_height
    twelfth = eleventh * inv_height
    parallel = 1.0 - 0.5625 * inv_height + 0.125 * cubed - 0.17578125 * fourth - 0.0625 * fifth
    perpend = (
        1.0
        - 1.125 * inv_height
        + 0.5 * cubed
        - 0.57 * fourth
        + 0.2 * fifth
        + 0.035 * eleventh
        - 0.04 * twelfth
    )
    return parallel, parallel, perpend


def kernel(
    sizes, local, width, counts_hbm, pos_hbm, gauss_hbm, out_ref,
    counts_ref, pos_ref, gauss_ref, load_sem, packed, mapped, halo_x, halo_y, halo_z, next_x, next_y, next_z,
    column, image_column, acc, iso, dyad, sums,
    send_one, recv_one, send_two, recv_two, send_sum, recv_sum, told_sem, line_sem,
):
    here = tuple(lax.axis_index(name) for name in names)
    cells = list(itertools.product(*(range(size) for size in local)))
    halos, nexts = (halo_x, halo_y, halo_z), (next_x, next_y, next_z)
    stages = groups_of(sizes)
    offsets = [stage_offsets(sizes, axes) for axes in stages]
    faces = [(axis, side) for axis in range(3) if sizes[axis] > 1 for side in range(2)]
    groups = width // lanes

    def exists(axis, side):
        return here[axis] < sizes[axis] - 1 if side else here[axis] > 0

    def slab(axis, side):
        index = [slice(None)] * 3
        index[axis] = pl.ds(local[axis] - 1 if side else 0, 1)
        return tuple(index)

    def beside(axis, side):
        return {names[axis]: here[axis] + (1 if side else -1)}

    loads = [
        pltpu.make_async_copy(source, target, load_sem.at[order])
        for order, (source, target) in enumerate(
            ((pos_hbm, pos_ref), (gauss_hbm, gauss_ref), (counts_hbm, counts_ref))
        )
    ]
    for load in loads:
        load.start()

    ring = around(here, sizes)

    def shifted(offset):
        return tuple(ring[k][offset[k]] for k in range(3))

    barrier = pltpu.get_barrier_semaphore()
    peers, near, told = entry_plan(sizes)
    if near:
        for side in range(2):
            pl.when(exists(2, side))(lambda s=side: pl.semaphore_signal(
                barrier, inc=1, device_id=beside(2, s), device_id_type=pl.DeviceIdType.MESH
            ))
    for offset in peers:
        pl.semaphore_signal(
            barrier, inc=1, device_id=shifted(offset),
            device_id_type=pl.DeviceIdType.MESH,
        )

    zero_tile = jnp.zeros((lanes, width), jnp.float32)
    tile_row = lax.broadcasted_iota(jnp.int32, (lanes, width), 0)
    outside = jnp.where(tile_row < 3, far_away, 0.0)
    for axis in range(3):
        face_cells = [c for c in cells if c[axis] == 0]
        for side in range(2):
            def clear(axis=axis, side=side, face_cells=face_cells):
                for cell in face_cells:
                    halos[axis][(side,) + cell] = outside
                    if side:
                        nexts[axis][cell] = zero_tile
            pl.when(jnp.logical_not(exists(axis, side)))(clear)

    for load in loads:
        load.wait()
    lane = lax.broadcasted_iota(jnp.int32, (1, width), 1)
    occupied, walls = {}, {}
    for cell in cells:
        occupied[cell] = (lane < counts_ref[cell]).astype(jnp.float32)
        for which in range(3):
            from_array = cell[:2] + (which, pl.ds(cell[2], 1))
            packed[cell + (pl.ds(which, 1),)] = pos_ref[from_array]
            packed[cell + (pl.ds(3 + which, 1),)] = gauss_ref[from_array] * occupied[cell]
        packed[cell + (pl.ds(6, 2),)] = jnp.zeros((2, width), jnp.float32)
        walls[cell] = wall_mobility(packed[cell + (pl.ds(2, 1),)])

    def row(ref, index, which):
        return ref[index + (pl.ds(which, 1),)]

    def spread(ref, cell, values):
        for which in range(3):
            full = jnp.broadcast_to(values[which], (width, width))
            ref[cell + (which,)] = full.T

    def source_of(cell, axis, side):
        there = list(cell)
        there[axis] += 1 if side else -1
        if 0 <= there[axis] < local[axis]:
            return packed, tuple(there), False
        there[axis] = 0
        return halos[axis], (side,) + tuple(there), True

    inner, outer, saved = {}, {}, []
    for cell in cells:
        inner[cell] = [(packed, cell, None)]
        outer[cell] = []
        saved.append((cell, None))
        for axis in range(3):
            for side in range(2):
                ref, index, remote = source_of(cell, axis, side)
                if remote and sizes[axis] == 1:
                    continue
                (outer if remote else inner)[cell].append((ref, index, (axis, side)))
                if side:
                    saved.append((cell, axis))
    slot_of = {key: slot for slot, key in enumerate(saved)}

    def diagonal(group):
        rows = group * lanes + lax.broadcasted_iota(jnp.int32, (lanes, width), 0)
        return rows == lax.broadcasted_iota(jnp.int32, (lanes, width), 1)

    def first_product(table, start):
        def body(group, carry):
            rows = pl.ds(pl.multiple_of(group * lanes, lanes), lanes)
            for cell in cells:
                target = [column[cell + (which, rows)] for which in range(3)]
                total = None if start else [acc[cell + (which, rows)] for which in range(3)]
                for ref, index, direction in table[cell]:
                    delta = [target[which] - row(ref, index, which) for which in range(3)]
                    value = [row(ref, index, 3 + which) for which in range(3)]
                    square = delta[0] * delta[0] + delta[1] * delta[1] + delta[2] * delta[2]
                    inverse = lax.rsqrt(square)
                    if direction is None:
                        inverse = jnp.where(diagonal(group), 0.0, inverse)
                    inv_sq = inverse * inverse
                    isotropic = inverse * (0.75 + 0.5 * inv_sq)
                    dyadic = (inverse * inv_sq) * (0.75 - 1.5 * inv_sq)
                    if direction is None or direction[1]:
                        slot = slot_of[(cell, None if direction is None else direction[0])]
                        iso[slot, rows] = isotropic
                        dyad[slot, rows] = dyadic
                    scaled = dyadic * (
                        delta[0] * value[0] + delta[1] * value[1] + delta[2] * value[2]
                    )
                    part = [isotropic * value[which] + delta[which] * scaled for which in range(3)]
                    total = part if total is None else [a + b for a, b in zip(total, part)]
                for which in range(3):
                    acc[cell + (which, rows)] = total[which]
            return carry

        lax.fori_loop(0, groups, body, 0)

    along_z = sum(jnp.where(exists(2, side), 1, 0) for side in range(2))
    pl.semaphore_wait(barrier, len(peers) + along_z if near else len(peers))

    def halo_copy(axis, side, receiver):
        held = side if receiver else 1 - side
        face = 2 * axis + held
        return pltpu.make_async_remote_copy(
            src_ref=packed.at[slab(axis, side)],
            dst_ref=halos[axis].at[held],
            send_sem=send_one.at[2 * axis + side],
            recv_sem=recv_one.at[face],
            device_id=beside(axis, side),
            device_id_type=pl.DeviceIdType.MESH,
        )

    def next_copy(axis, side):
        return pltpu.make_async_remote_copy(
            src_ref=mapped.at[slab(axis, 0)],
            dst_ref=nexts[axis],
            send_sem=send_two.at[axis],
            recv_sem=recv_two.at[axis],
            device_id=beside(axis, side),
            device_id_type=pl.DeviceIdType.MESH,
        )

    for axis, side in faces:
        pl.when(exists(axis, side))(lambda a=axis, s=side: halo_copy(a, s, False).start())
    for cell in cells:
        spread(column, cell, [row(packed, cell, which) for which in range(3)])

    first_product(inner, True)

    for axis, side in faces:
        pl.when(exists(axis, side))(lambda a=axis, s=side: halo_copy(a, s, True).wait_recv())

    if near:
        for side in range(2):
            pl.when(exists(2, side))(lambda s=side: pl.semaphore_signal(
                line_sem, inc=1, device_id=beside(2, s), device_id_type=pl.DeviceIdType.MESH
            ))

    first_product(outer, False)

    images = {}
    for cell in cells:
        images[cell] = []
        for which in range(3):
            summed = jnp.sum(acc[cell + (which,)].T, axis=0, keepdims=True)
            value = row(packed, cell, 3 + which)
            image = (walls[cell][which] * value + summed) * occupied[cell]
            images[cell].append(image)
            mapped[cell + (pl.ds(which, 1),)] = image
        mapped[cell + (pl.ds(3, lanes - 3),)] = jnp.zeros((lanes - 3, width), jnp.float32)

    for axis in range(3):
        if sizes[axis] > 1:
            pl.when(exists(axis, 0))(lambda a=axis: next_copy(a, 0).start())

    if near:
        pl.semaphore_wait(line_sem, along_z)
    for offset in told:
        pl.semaphore_signal(
            told_sem, inc=1, device_id=shifted(offset), device_id_type=pl.DeviceIdType.MESH
        )

    for cell in cells:
        spread(image_column, cell, images[cell])

    def other_of(cell, axis):
        there = list(cell)
        if axis is None:
            return packed, cell, mapped, cell
        there[axis] += 1
        if there[axis] < local[axis]:
            return packed, tuple(there), mapped, tuple(there)
        there[axis] = 0
        return halos[axis], (1,) + tuple(there), nexts[axis], tuple(there)

    blocks = [
        key for key in saved
        if key[1] is None or key[0][key[1]] + 1 < local[key[1]] or sizes[key[1]] > 1
    ]

    def second_body(group, carry):
        rows = pl.ds(pl.multiple_of(group * lanes, lanes), lanes)
        result = []
        for (cell, axis), total in zip(blocks, carry):
            place, index, _, _ = other_of(cell, axis)
            slot = slot_of[(cell, axis)]
            delta = [
                column[cell + (which, rows)] - row(place, index, which) for which in range(3)
            ]
            value = [image_column[cell + (which, rows)] for which in range(3)]
            isotropic = iso[slot, rows]
            scaled = dyad[slot, rows] * (
                delta[0] * value[0] + delta[1] * value[1] + delta[2] * value[2]
            )
            result.append(tuple(
                total[which] + isotropic * value[which] + delta[which] * scaled
                for which in range(3)
            ))
        return tuple(result)

    zero = (jnp.zeros((lanes, width), jnp.float32),) * 3
    pushed = lax.fori_loop(0, groups, second_body, (zero,) * len(blocks))

    noise_sq = cross_one = image_sq = wall_sq = jnp.zeros((1, width), jnp.float32)
    for cell in cells:
        for which in range(3):
            value, image = row(packed, cell, 3 + which), images[cell][which]
            noise_sq += value * value
            cross_one += value * image
            image_sq += image * image
            wall_sq += walls[cell][which] * image * image

    own_pairs = jnp.zeros((lanes, width), jnp.float32)
    remote = []
    for (cell, axis), total in zip(blocks, pushed):
        _, _, vector, index = other_of(cell, axis)
        if axis is not None and cell[axis] + 1 == local[axis]:
            remote.append((vector, index, total))
            continue
        weight = 1.0 if axis is None else 2.0
        for which in range(3):
            own_pairs += weight * total[which] * row(vector, index, which)

    for axis in range(3):
        if sizes[axis] > 1:
            pl.when(exists(axis, 1))(lambda a=axis: next_copy(a, 1).wait_recv())

    for vector, index, total in remote:
        for which in range(3):
            own_pairs += 2.0 * total[which] * row(vector, index, which)
    cross_two = wall_sq + jnp.sum(own_pairs, axis=0, keepdims=True)

    sublane = lax.broadcasted_iota(jnp.int32, (lanes, width), 0)
    tile = jnp.where(sublane == 0, noise_sq, 0.0)
    for which, part in enumerate((cross_one, image_sq, cross_two)):
        tile = jnp.where(sublane == which + 1, part, tile)
    reduced = jnp.broadcast_to(jnp.sum(tile, axis=1, keepdims=True), (lanes, width))
    chosen = sublane == lax.broadcasted_iota(jnp.int32, (lanes, width), 1)
    partial = jnp.sum(jnp.where(chosen, reduced, 0.0), axis=0, keepdims=True)

    if told:
        pl.semaphore_wait(told_sem, len(told))
    base = 0
    for number, stage in enumerate(offsets):
        count = len(stage)
        if count == 0:
            continue
        position = {offset: base + order for order, offset in enumerate(stage)}
        own = base + count
        sums[pl.ds(own, 1)] = partial
        copies = []
        for offset in stage:
            back = tuple((sizes[k] - offset[k]) % sizes[k] for k in range(3))
            copy = pltpu.make_async_remote_copy(
                src_ref=sums.at[pl.ds(own, 1)],
                dst_ref=sums.at[pl.ds(position[back], 1)],
                send_sem=send_sum.at[position[offset]],
                recv_sem=recv_sum.at[position[back]],
                device_id=shifted(offset),
                device_id_type=pl.DeviceIdType.MESH,
            )
            copy.start()
            copies.append((offset, copy))
        for offset, _ in copies:
            pltpu.make_async_remote_copy(
                src_ref=sums.at[pl.ds(own, 1)],
                dst_ref=sums.at[pl.ds(position[offset], 1)],
                send_sem=send_sum.at[position[offset]],
                recv_sem=recv_sum.at[position[offset]],
                device_id=shifted(offset),
                device_id_type=pl.DeviceIdType.MESH,
            ).wait_recv()
        partial = jnp.sum(sums[pl.ds(base, count + 1)], axis=0, keepdims=True)
        for _, copy in copies:
            copy.wait_send()
        base += -(-(count + 1) // lanes) * lanes

    def scalar(which):
        return jnp.sum(jnp.where(lane == which, partial, 0.0), axis=1, keepdims=True)

    noise, cross, image_norm, cross_next = (scalar(which) for which in range(4))
    alpha_one = cross / noise
    beta_sq = image_norm / noise - alpha_one * alpha_one
    alpha_two = (
        cross_next - 2.0 * alpha_one * image_norm + alpha_one * alpha_one * cross
    ) / (noise * beta_sq)
    root_det = jnp.sqrt(alpha_one * alpha_two - beta_sq)
    trace_root = jnp.sqrt(alpha_one + alpha_two + 2.0 * root_det)
    image_factor = 1.0 / trace_root
    noise_factor = root_det * image_factor
    for cell in cells:
        for which in range(3):
            out_ref[cell[:2] + (which, pl.ds(cell[2], 1))] = (
                noise_factor * row(packed, cell, 3 + which)
                + image_factor * row(mapped, cell, which)
            )

    for axis, side in faces:
        pl.when(exists(axis, side))(lambda a=axis, s=side: halo_copy(a, s, False).wait_send())
    for axis in range(3):
        if sizes[axis] > 1:
            pl.when(exists(axis, 0))(lambda a=axis: next_copy(a, 0).wait_send())


def shards(sizes, positions, gaussian, counts):
    local, width = positions.shape[:3], positions.shape[-1]
    cells = local[0] * local[1] * local[2]
    f32 = jnp.float32
    vmem = lambda *shape: pltpu.VMEM(shape, f32)
    sem = lambda count: pltpu.SemaphoreType.DMA((count,))
    slabs = [tuple(1 if k == axis else local[k] for k in range(3)) for axis in range(3)]
    rows = sum(
        -(-(len(stage_offsets(sizes, axes)) + 1) // lanes) * lanes for axes in groups_of(sizes)
    )
    order = (0, 1, 3, 2, 4)
    positions, gaussian = (jnp.transpose(array, order) for array in (positions, gaussian))
    result = pl.pallas_call(
        functools.partial(kernel, sizes, local, width),
        out_shape=pltpu.VMEM(positions.shape, f32),
        in_specs=[pl.BlockSpec(memory_space=pltpu.HBM)] * 3,
        out_specs=pl.BlockSpec(memory_space=pltpu.VMEM),
        scratch_shapes=[
            pltpu.SMEM(counts.shape, jnp.int32),
            vmem(*positions.shape),
            vmem(*positions.shape),
            sem(3),
            vmem(*local, lanes, width),
            vmem(*local, lanes, width),
            *(vmem(2, *slab, lanes, width) for slab in slabs),
            *(vmem(*slab, lanes, width) for slab in slabs),
            vmem(*local, 3, width, width),
            vmem(*local, 3, width, width),
            vmem(*local, 3, width, width),
            vmem(4 * cells, width, width),
            vmem(4 * cells, width, width),
            vmem(rows, width),
            sem(6), sem(6), sem(3), sem(3), sem(rows), sem(rows), pltpu.SemaphoreType.REGULAR, pltpu.SemaphoreType.REGULAR,
        ],
        compiler_params=pltpu.CompilerParams(collective_id=0, has_side_effects=True),
    )(counts, positions, gaussian)
    return jnp.transpose(result, order)


def solution(mesh):
    sizes = tuple(mesh.shape[name] for name in names)
    in_specs = (
        P("gx", "gy", "gz", None, None),
        P("gx", "gy", "gz", None, None),
        P("gx", "gy", "gz"),
    )
    out_specs = P("gx", "gy", "gz", None, None)
    return jax.shard_map(
        functools.partial(shards, sizes), mesh=mesh, in_specs=in_specs, out_specs=out_specs,
        check_vma=False,
    )
```

```python
import functools
import itertools

import jax
import jax.numpy as jnp
from jax import lax
from jax.experimental import pallas as pl
from jax.experimental.pallas import tpu as pltpu
from jax.sharding import PartitionSpec as P

wall_gap = 1.0
lanes = 8
direct_limit = 64
far_away = -4096.0
names = ("gx", "gy", "gz")


def groups_of(sizes):
    total = sizes[0] * sizes[1] * sizes[2]
    return [(0, 1, 2)] if total <= direct_limit else [(0,), (1,), (2,)]


def stage_offsets(sizes, axes):
    ranges = [range(sizes[k]) if k in axes else range(1) for k in range(3)]
    away = lambda offset: sum(min(o, size - o) for o, size in zip(offset, sizes))
    found = [offset for offset in itertools.product(*ranges) if any(offset)]
    return sorted(found, key=away, reverse=True)


def entry_plan(sizes):
    stages = groups_of(sizes)
    if len(stages) > 1:
        return [offset for axes in stages for offset in stage_offsets(sizes, axes)], False, []
    near = 1 < sizes[2] <= 4
    lines = stage_offsets(sizes, (0,)) + stage_offsets(sizes, (1,))
    plane = stage_offsets(sizes, (0, 1))
    return (lines if near else plane + stage_offsets(sizes, (2,))), near, plane


def around(here, sizes):
    table = []
    for k in range(3):
        ahead = [here[k] + step for step in range(sizes[k])]
        table.append([jnp.where(at >= sizes[k], at - sizes[k], at) for at in ahead])
    return table


def wall_mobility(height):
    inv_height = 1.0 / (height + wall_gap)
    squared = inv_height * inv_height
    cubed = squared * inv_height
    fourth = squared * squared
    fifth = fourth * inv_height
    eleventh = fifth * fifth * inv_height
    twelfth = eleventh * inv_height
    parallel = 1.0 - 0.5625 * inv_height + 0.125 * cubed - 0.17578125 * fourth - 0.0625 * fifth
    perpend = (
        1.0
        - 1.125 * inv_height
        + 0.5 * cubed
        - 0.57 * fourth
        + 0.2 * fifth
        + 0.035 * eleventh
        - 0.04 * twelfth
    )
    return parallel, parallel, perpend


def kernel(
    sizes, local, width, counts_hbm, pos_hbm, gauss_hbm, out_ref,
    counts_ref, pos_ref, gauss_ref, load_sem, packed, mapped, halo_x, halo_y, halo_z, next_x, next_y, next_z,
    column, image_column, acc, iso, dyad, sums,
    send_one, recv_one, send_two, recv_two, send_sum, recv_sum, told_sem, line_sem,
):
    here = tuple(lax.axis_index(name) for name in names)
    cells = list(itertools.product(*(range(size) for size in local)))
    halos, nexts = (halo_x, halo_y, halo_z), (next_x, next_y, next_z)
    stages = groups_of(sizes)
    offsets = [stage_offsets(sizes, axes) for axes in stages]
    faces = [(axis, side) for axis in range(3) if sizes[axis] > 1 for side in range(2)]
    groups = width // lanes

    def exists(axis, side):
        return here[axis] < sizes[axis] - 1 if side else here[axis] > 0

    def slab(axis, side):
        index = [slice(None)] * 3
        index[axis] = pl.ds(local[axis] - 1 if side else 0, 1)
        return tuple(index)

    def beside(axis, side):
        return {names[axis]: here[axis] + (1 if side else -1)}

    loads = [
        pltpu.make_async_copy(source, target, load_sem.at[order])
        for order, (source, target) in enumerate(
            ((pos_hbm, pos_ref), (gauss_hbm, gauss_ref), (counts_hbm, counts_ref))
        )
    ]
    for load in loads:
        load.start()

    ring = around(here, sizes)

    def shifted(offset):
        return tuple(ring[k][offset[k]] for k in range(3))

    barrier = pltpu.get_barrier_semaphore()
    peers, near, told = entry_plan(sizes)
    if near:
        for side in range(2):
            pl.when(exists(2, side))(lambda s=side: pl.semaphore_signal(
                barrier, inc=1, device_id=beside(2, s), device_id_type=pl.DeviceIdType.MESH
            ))
    for offset in peers:
        pl.semaphore_signal(
            barrier, inc=1, device_id=shifted(offset),
            device_id_type=pl.DeviceIdType.MESH,
        )

    zero_tile = jnp.zeros((lanes, width), jnp.float32)
    tile_row = lax.broadcasted_iota(jnp.int32, (lanes, width), 0)
    outside = jnp.where(tile_row < 3, far_away, 0.0)
    for axis in range(3):
        face_cells = [c for c in cells if c[axis] == 0]
        for side in range(2):
            def clear(axis=axis, side=side, face_cells=face_cells):
                for cell in face_cells:
                    halos[axis][(side,) + cell] = outside
                    if side:
                        nexts[axis][cell] = zero_tile
            pl.when(jnp.logical_not(exists(axis, side)))(clear)

    for load in loads:
        load.wait()
    lane = lax.broadcasted_iota(jnp.int32, (1, width), 1)
    occupied, walls = {}, {}
    for cell in cells:
        occupied[cell] = (lane < counts_ref[cell]).astype(jnp.float32)
        for which in range(3):
            from_array = cell[:2] + (which, pl.ds(cell[2], 1))
            packed[cell + (pl.ds(which, 1),)] = pos_ref[from_array]
            packed[cell + (pl.ds(3 + which, 1),)] = gauss_ref[from_array] * occupied[cell]
        packed[cell + (pl.ds(6, 2),)] = jnp.zeros((2, width), jnp.float32)
        walls[cell] = wall_mobility(packed[cell + (pl.ds(2, 1),)])

    def row(ref, index, which):
        return ref[index + (pl.ds(which, 1),)]

    def spread(ref, cell, values):
        for which in range(3):
            full = jnp.broadcast_to(values[which], (width, width))
            ref[cell + (which,)] = full.T

    def source_of(cell, axis, side):
        there = list(cell)
        there[axis] += 1 if side else -1
        if 0 <= there[axis] < local[axis]:
            return packed, tuple(there), False
        there[axis] = 0
        return halos[axis], (side,) + tuple(there), True

    inner, outer, saved = {}, {}, []
    for cell in cells:
        inner[cell] = [(packed, cell, None)]
        outer[cell] = []
        saved.append((cell, None))
        for axis in range(3):
            for side in range(2):
                ref, index, remote = source_of(cell, axis, side)
                if remote and sizes[axis] == 1:
                    continue
                (outer if remote else inner)[cell].append((ref, index, (axis, side)))
                if side:
                    saved.append((cell, axis))
    slot_of = {key: slot for slot, key in enumerate(saved)}

    def diagonal(group):
        rows = group * lanes + lax.broadcasted_iota(jnp.int32, (lanes, width), 0)
        return rows == lax.broadcasted_iota(jnp.int32, (lanes, width), 1)

    def first_product(table, start):
        def body(group, carry):
            rows = pl.ds(pl.multiple_of(group * lanes, lanes), lanes)
            for cell in cells:
                target = [column[cell + (which, rows)] for which in range(3)]
                total = None if start else [acc[cell + (which, rows)] for which in range(3)]
                for ref, index, direction in table[cell]:
                    delta = [target[which] - row(ref, index, which) for which in range(3)]
                    value = [row(ref, index, 3 + which) for which in range(3)]
                    square = delta[0] * delta[0] + delta[1] * delta[1] + delta[2] * delta[2]
                    inverse = lax.rsqrt(square)
                    if direction is None:
                        inverse = jnp.where(diagonal(group), 0.0, inverse)
                    inv_sq = inverse * inverse
                    isotropic = inverse * (0.75 + 0.5 * inv_sq)
                    dyadic = (inverse * inv_sq) * (0.75 - 1.5 * inv_sq)
                    if direction is None or direction[1]:
                        slot = slot_of[(cell, None if direction is None else direction[0])]
                        iso[slot, rows] = isotropic
                        dyad[slot, rows] = dyadic
                    scaled = dyadic * (
                        delta[0] * value[0] + delta[1] * value[1] + delta[2] * value[2]
                    )
                    part = [isotropic * value[which] + delta[which] * scaled for which in range(3)]
                    total = part if total is None else [a + b for a, b in zip(total, part)]
                for which in range(3):
                    acc[cell + (which, rows)] = total[which]
            return carry

        lax.fori_loop(0, groups, body, 0, unroll=4)

    along_z = sum(jnp.where(exists(2, side), 1, 0) for side in range(2))
    pl.semaphore_wait(barrier, len(peers) + along_z if near else len(peers))

    def halo_copy(axis, side, receiver):
        held = side if receiver else 1 - side
        face = 2 * axis + held
        return pltpu.make_async_remote_copy(
            src_ref=packed.at[slab(axis, side)],
            dst_ref=halos[axis].at[held],
            send_sem=send_one.at[2 * axis + side],
            recv_sem=recv_one.at[face],
            device_id=beside(axis, side),
            device_id_type=pl.DeviceIdType.MESH,
        )

    def next_copy(axis, side):
        return pltpu.make_async_remote_copy(
            src_ref=mapped.at[slab(axis, 0)],
            dst_ref=nexts[axis],
            send_sem=send_two.at[axis],
            recv_sem=recv_two.at[axis],
            device_id=beside(axis, side),
            device_id_type=pl.DeviceIdType.MESH,
        )

    for axis, side in faces:
        pl.when(exists(axis, side))(lambda a=axis, s=side: halo_copy(a, s, False).start())
    for cell in cells:
        spread(column, cell, [row(packed, cell, which) for which in range(3)])

    first_product(inner, True)

    for axis, side in faces:
        pl.when(exists(axis, side))(lambda a=axis, s=side: halo_copy(a, s, True).wait_recv())

    if near:
        for side in range(2):
            pl.when(exists(2, side))(lambda s=side: pl.semaphore_signal(
                line_sem, inc=1, device_id=beside(2, s), device_id_type=pl.DeviceIdType.MESH
            ))

    first_product(outer, False)

    images = {}
    for cell in cells:
        images[cell] = []
        for which in range(3):
            summed = jnp.sum(acc[cell + (which,)].T, axis=0, keepdims=True)
            value = row(packed, cell, 3 + which)
            image = (walls[cell][which] * value + summed) * occupied[cell]
            images[cell].append(image)
            mapped[cell + (pl.ds(which, 1),)] = image
        mapped[cell + (pl.ds(3, lanes - 3),)] = jnp.zeros((lanes - 3, width), jnp.float32)

    for axis in range(3):
        if sizes[axis] > 1:
            pl.when(exists(axis, 0))(lambda a=axis: next_copy(a, 0).start())

    if near:
        pl.semaphore_wait(line_sem, along_z)
    for offset in told:
        pl.semaphore_signal(
            told_sem, inc=1, device_id=shifted(offset), device_id_type=pl.DeviceIdType.MESH
        )

    for cell in cells:
        spread(image_column, cell, images[cell])

    def other_of(cell, axis):
        there = list(cell)
        if axis is None:
            return packed, cell, mapped, cell
        there[axis] += 1
        if there[axis] < local[axis]:
            return packed, tuple(there), mapped, tuple(there)
        there[axis] = 0
        return halos[axis], (1,) + tuple(there), nexts[axis], tuple(there)

    blocks = [
        key for key in saved
        if key[1] is None or key[0][key[1]] + 1 < local[key[1]] or sizes[key[1]] > 1
    ]

    def second_body(group, carry):
        rows = pl.ds(pl.multiple_of(group * lanes, lanes), lanes)
        result = []
        for (cell, axis), total in zip(blocks, carry):
            place, index, _, _ = other_of(cell, axis)
            slot = slot_of[(cell, axis)]
            delta = [
                column[cell + (which, rows)] - row(place, index, which) for which in range(3)
            ]
            value = [image_column[cell + (which, rows)] for which in range(3)]
            isotropic = iso[slot, rows]
            scaled = dyad[slot, rows] * (
                delta[0] * value[0] + delta[1] * value[1] + delta[2] * value[2]
            )
            result.append(tuple(
                total[which] + isotropic * value[which] + delta[which] * scaled
                for which in range(3)
            ))
        return tuple(result)

    zero = (jnp.zeros((lanes, width), jnp.float32),) * 3
    pushed = lax.fori_loop(0, groups, second_body, (zero,) * len(blocks), unroll=4)

    noise_sq = cross_one = image_sq = wall_sq = jnp.zeros((1, width), jnp.float32)
    for cell in cells:
        for which in range(3):
            value, image = row(packed, cell, 3 + which), images[cell][which]
            noise_sq += value * value
            cross_one += value * image
            image_sq += image * image
            wall_sq += walls[cell][which] * image * image

    own_pairs = jnp.zeros((lanes, width), jnp.float32)
    remote = []
    for (cell, axis), total in zip(blocks, pushed):
        _, _, vector, index = other_of(cell, axis)
        if axis is not None and cell[axis] + 1 == local[axis]:
            remote.append((vector, index, total))
            continue
        weight = 1.0 if axis is None else 2.0
        for which in range(3):
            own_pairs += weight * total[which] * row(vector, index, which)

    for axis in range(3):
        if sizes[axis] > 1:
            pl.when(exists(axis, 1))(lambda a=axis: next_copy(a, 1).wait_recv())

    for vector, index, total in remote:
        for which in range(3):
            own_pairs += 2.0 * total[which] * row(vector, index, which)
    cross_two = wall_sq + jnp.sum(own_pairs, axis=0, keepdims=True)

    sublane = lax.broadcasted_iota(jnp.int32, (lanes, width), 0)
    tile = jnp.where(sublane == 0, noise_sq, 0.0)
    for which, part in enumerate((cross_one, image_sq, cross_two)):
        tile = jnp.where(sublane == which + 1, part, tile)
    reduced = jnp.broadcast_to(jnp.sum(tile, axis=1, keepdims=True), (lanes, width))
    chosen = sublane == lax.broadcasted_iota(jnp.int32, (lanes, width), 1)
    partial = jnp.sum(jnp.where(chosen, reduced, 0.0), axis=0, keepdims=True)

    if told:
        pl.semaphore_wait(told_sem, len(told))
    base = 0
    for number, stage in enumerate(offsets):
        count = len(stage)
        if count == 0:
            continue
        position = {offset: base + order for order, offset in enumerate(stage)}
        own = base + count
        sums[pl.ds(own, 1)] = partial
        copies = []
        for offset in stage:
            back = tuple((sizes[k] - offset[k]) % sizes[k] for k in range(3))
            copy = pltpu.make_async_remote_copy(
                src_ref=sums.at[pl.ds(own, 1)],
                dst_ref=sums.at[pl.ds(position[back], 1)],
                send_sem=send_sum.at[position[offset]],
                recv_sem=recv_sum.at[position[back]],
                device_id=shifted(offset),
                device_id_type=pl.DeviceIdType.MESH,
            )
            copy.start()
            copies.append((offset, copy))
        for offset, _ in copies:
            pltpu.make_async_remote_copy(
                src_ref=sums.at[pl.ds(own, 1)],
                dst_ref=sums.at[pl.ds(position[offset], 1)],
                send_sem=send_sum.at[position[offset]],
                recv_sem=recv_sum.at[position[offset]],
                device_id=shifted(offset),
                device_id_type=pl.DeviceIdType.MESH,
            ).wait_recv()
        partial = jnp.sum(sums[pl.ds(base, count + 1)], axis=0, keepdims=True)
        for _, copy in copies:
            copy.wait_send()
        base += -(-(count + 1) // lanes) * lanes

    def scalar(which):
        return jnp.sum(jnp.where(lane == which, partial, 0.0), axis=1, keepdims=True)

    noise, cross, image_norm, cross_next = (scalar(which) for which in range(4))
    alpha_one = cross / noise
    beta_sq = image_norm / noise - alpha_one * alpha_one
    alpha_two = (
        cross_next - 2.0 * alpha_one * image_norm + alpha_one * alpha_one * cross
    ) / (noise * beta_sq)
    root_det = jnp.sqrt(alpha_one * alpha_two - beta_sq)
    trace_root = jnp.sqrt(alpha_one + alpha_two + 2.0 * root_det)
    image_factor = 1.0 / trace_root
    noise_factor = root_det * image_factor
    for cell in cells:
        for which in range(3):
            out_ref[cell[:2] + (which, pl.ds(cell[2], 1))] = (
                noise_factor * row(packed, cell, 3 + which)
                + image_factor * row(mapped, cell, which)
            )

    for axis, side in faces:
        pl.when(exists(axis, side))(lambda a=axis, s=side: halo_copy(a, s, False).wait_send())
    for axis in range(3):
        if sizes[axis] > 1:
            pl.when(exists(axis, 0))(lambda a=axis: next_copy(a, 0).wait_send())


def shards(sizes, positions, gaussian, counts):
    local, width = positions.shape[:3], positions.shape[-1]
    cells = local[0] * local[1] * local[2]
    f32 = jnp.float32
    vmem = lambda *shape: pltpu.VMEM(shape, f32)
    sem = lambda count: pltpu.SemaphoreType.DMA((count,))
    slabs = [tuple(1 if k == axis else local[k] for k in range(3)) for axis in range(3)]
    rows = sum(
        -(-(len(stage_offsets(sizes, axes)) + 1) // lanes) * lanes for axes in groups_of(sizes)
    )
    order = (0, 1, 3, 2, 4)
    positions, gaussian = (jnp.transpose(array, order) for array in (positions, gaussian))
    result = pl.pallas_call(
        functools.partial(kernel, sizes, local, width),
        out_shape=pltpu.VMEM(positions.shape, f32),
        in_specs=[pl.BlockSpec(memory_space=pltpu.HBM)] * 3,
        out_specs=pl.BlockSpec(memory_space=pltpu.VMEM),
        scratch_shapes=[
            pltpu.SMEM(counts.shape, jnp.int32),
            vmem(*positions.shape),
            vmem(*positions.shape),
            sem(3),
            vmem(*local, lanes, width),
            vmem(*local, lanes, width),
            *(vmem(2, *slab, lanes, width) for slab in slabs),
            *(vmem(*slab, lanes, width) for slab in slabs),
            vmem(*local, 3, width, width),
            vmem(*local, 3, width, width),
            vmem(*local, 3, width, width),
            vmem(4 * cells, width, width),
            vmem(4 * cells, width, width),
            vmem(rows, width),
            sem(6), sem(6), sem(3), sem(3), sem(rows), sem(rows), pltpu.SemaphoreType.REGULAR, pltpu.SemaphoreType.REGULAR,
        ],
        compiler_params=pltpu.CompilerParams(collective_id=0, has_side_effects=True),
    )(counts, positions, gaussian)
    return jnp.transpose(result, order)


def solution(mesh):
    sizes = tuple(mesh.shape[name] for name in names)
    in_specs = (
        P("gx", "gy", "gz", None, None),
        P("gx", "gy", "gz", None, None),
        P("gx", "gy", "gz"),
    )
    out_specs = P("gx", "gy", "gz", None, None)
    return jax.shard_map(
        functools.partial(shards, sizes), mesh=mesh, in_specs=in_specs, out_specs=out_specs,
        check_vma=False,
    )
```
